32 devices in a mesh: section: 8 (over z, core), row: 4 (over y, x).
Axes of the slice: x: 2, y: 2, z: 4, core: 2. Of those that a mesh axis runs over, the one named last changes fastest.
Arguments:
- section_inputs: bfloat16 [8, 512, 2048], P('section', 'row'), may hold values from -6 to 6
- fresh_group: bfloat16 [512, 2048], P('row'), may hold values from -6 to 6
- resident_state: float32 [8, 8, 128, 128], P('section'), may hold values from -81.4587 to 81.4587
- qkv_weight: bfloat16 [8, 2048, 3072], P('section', 'row'), may hold values from -0.125 to 0.125
- out_weight: bfloat16 [8, 1024, 2048], P('section', 'row'), may hold values from -0.1875 to 0.1875
- input_gain: float32 [8, 2048], P('section'), may hold values from 0.1 to 1.9
- head_gain: float32 [8, 1024], P('section'), may hold values from 0.1 to 1.9
Outputs:
- section_outputs: bfloat16 [8, 512, 2048], P('section', 'row')
- final_state: float32 [8, 8, 128, 128], P('section')
The draws below stay inside these ranges and needn't reach their ends.
All inputs are finite; a program needn't handle non-finite values.
Results may differ from the reference program's by a relative error of at most 0.01.
Values may be sent and summed in bfloat16 or wider, within the bound.
No kernel may reach another device: no remote copies, remote signals or barrier semaphores. Data moves between devices by JAX's collectives and lax.ppermute only.
A program may use at most 64 MiB of HBM per device.

```python
import jax
import jax.numpy as jnp
from jax import lax

D = 2048
HEADS = 8
HEAD = 128
ROWS_DEV = 128
SECTIONS = 8
GROUP = 512
N_ROW = 4


def steps_of(key, extent, split, least, top_value):
    def one(position, shards_of):
        steps = jax.random.uniform(jax.random.fold_in(jax.random.fold_in(key, 6), position), (shards_of,), jnp.float32, least / len(split), top_value / len(split))
        return jnp.repeat(jnp.exp(steps), extent[position] // shards_of).reshape((-1,) + (1,) * (len(extent) - position - 1))

    level = one(*split[0])
    for cut in split[1:]:
        level = level * one(*cut)
    return level


def scatter_about(own_key, shape, scale, bound, cuts=(), held_as=jnp.bfloat16):
    array = scale * jax.random.normal(own_key, shape, jnp.float32)
    if cuts:
        array = array * steps_of(own_key, shape, cuts, -0.22, 0.18)
    return jnp.clip(array, -bound, bound).astype(held_as)


def setup_inputs(seed: int = 0) -> dict:
    splits = jax.random.split(jax.random.key(seed), 8)
    return {
        "section_inputs": scatter_about(splits[0], (SECTIONS, GROUP, D), 1.0, 6.0, ((0, 8), (1, 4))),
        "fresh_group": scatter_about(splits[1], (GROUP, D), 1.0, 6.0, ((0, 4),)),
        "resident_state": scatter_about(splits[2], (SECTIONS, HEADS, HEAD, HEAD), (0.6 * (ROWS_DEV * N_ROW) ** 0.5), 81.4587, ((0, 8),), jnp.float32),
        "qkv_weight": scatter_about(splits[3], (SECTIONS, D, 3 * HEADS * HEAD), D ** -0.5, 0.125, ((0, 8), (1, 4))),
        "out_weight": scatter_about(splits[4], (SECTIONS, HEADS * HEAD, D), (HEADS * HEAD) ** -0.5, 0.1875, ((0, 8), (1, 4))),
        "input_gain": jnp.clip(1.0 + 0.18 * jax.random.normal(splits[5], (SECTIONS, D), jnp.float32), 0.1, 1.9),
        "head_gain": jnp.clip(1.0 + 0.18 * jax.random.normal(splits[6], (SECTIONS, HEADS * HEAD), jnp.float32), 0.1, 1.9),
    }


def layer(inputs, state, qkv_weight, out_weight, input_gain, head_gain):
    width = HEADS * HEAD
    highest = lax.Precision.HIGHEST
    wide = inputs.astype(jnp.float32)
    normed = (wide * lax.rsqrt(lax.optimization_barrier(jnp.mean(wide * wide, axis=-1, keepdims=True)) + 1e-05) * input_gain).astype(jnp.bfloat16)
    projected = jnp.dot(normed, qkv_weight, preferred_element_type=jnp.float32)
    queries = jax.nn.silu(projected[:, :width]).astype(jnp.bfloat16)
    key_rows = jax.nn.silu(projected[:, width:2 * width]).astype(jnp.bfloat16)
    value_rows = projected[:, 2 * width:].astype(jnp.bfloat16)
    shape = (N_ROW, ROWS_DEV, HEADS, HEAD)
    query_blocks = queries.reshape(shape).astype(jnp.float32)
    key_blocks = key_rows.reshape(shape).astype(jnp.float32)
    value_blocks = value_rows.reshape(shape).astype(jnp.float32)
    block_state = jnp.einsum('bjhd,bjhe->bhde', key_blocks, value_blocks, precision=highest)
    running = jnp.cumsum(block_state, axis=0)
    before = jnp.concatenate([jnp.zeros_like(block_state[:1]), running[:-1]], axis=0)
    prefix = state[None] + before
    carried = jnp.einsum('bihd,bhde->bihe', query_blocks, prefix, precision=highest)
    scores = jnp.einsum('bihd,bjhd->bhij', query_blocks, key_blocks, precision=highest)
    causal = jnp.tril(jnp.ones((ROWS_DEV, ROWS_DEV), dtype=bool))
    weights = jnp.where(causal, scores, 0.0).astype(jnp.bfloat16)
    weights_back = lax.optimization_barrier(weights).astype(jnp.float32)
    local = jnp.einsum('bhij,bjhe->bihe', weights_back, value_blocks, precision=highest)
    attended = (carried + local).reshape(N_ROW * ROWS_DEV, HEADS, HEAD)
    scaled = attended * lax.rsqrt(lax.optimization_barrier(jnp.mean(attended * attended, axis=-1, keepdims=True)) + 1e-06)
    head_out = (scaled.reshape(N_ROW * ROWS_DEV, width) * head_gain).astype(jnp.bfloat16)
    result = (wide + jnp.dot(head_out, out_weight, preferred_element_type=jnp.float32)).astype(jnp.bfloat16)
    return (result, state + lax.optimization_barrier(jnp.sum(block_state, axis=0)))

def one_section(packed):
    return layer(*packed)

def reference(section_inputs, fresh_group, resident_state, qkv_weight, out_weight, input_gain, head_gain):
    first_out, first_state = lax.map(one_section, (section_inputs, resident_state, qkv_weight, out_weight, input_gain, head_gain))
    second_in = jnp.concatenate([fresh_group[None], first_out[:-1]], axis=0)
    section_outputs, final_state = lax.map(one_section, (second_in, first_state, qkv_weight, out_weight, input_gain, head_gain))
    return (section_outputs, final_state)
```

```python
import functools

import jax
import jax.numpy as jnp
from jax import lax
from jax.experimental import pallas as pl
from jax.experimental.pallas import tpu as pltpu
from jax.sharding import PartitionSpec as P


VMEM = pl.BlockSpec(memory_space=pltpu.VMEM)
SMEM = pl.BlockSpec(memory_space=pltpu.SMEM)
F32 = jnp.float32
BF16 = jnp.bfloat16


def passed_along(value, axis, by):
    peers = lax.axis_size(axis)
    pairs = [(i, i + by) for i in range(peers) if 0 <= i + by < peers]
    return lax.ppermute(value, axis, pairs)


def layer(inputs, state, qkv_full, out_full, input_gain, head_gain):
    rows = inputs.shape[0]
    heads = state.shape[0]
    head_size = state.shape[1]
    width = heads * head_size
    highest = lax.Precision.HIGHEST
    wide = inputs.astype(F32)
    normed = (
        wide * lax.rsqrt(jnp.mean(wide * wide, axis=-1, keepdims=True) + 1e-05) * input_gain
    ).astype(BF16)
    projected = jnp.dot(normed, qkv_full, preferred_element_type=F32)
    queries = jax.nn.silu(projected[:, :width]).astype(BF16).reshape(rows, heads, head_size)
    key_rows = (
        jax.nn.silu(projected[:, width : 2 * width]).astype(BF16).reshape(rows, heads, head_size)
    )
    value_rows = projected[:, 2 * width :].astype(BF16).reshape(rows, heads, head_size)
    own_state = jnp.einsum("jhd,jhe->hde", key_rows, value_rows, preferred_element_type=F32)
    every = lax.all_gather(own_state[None].astype(BF16), "row", axis=0, tiled=True).astype(F32)
    order = lax.iota(jnp.int32, every.shape[0])
    earlier = (order < lax.axis_index("row")).astype(F32)
    before = jnp.sum(every * earlier[:, None, None, None], axis=0)
    total = jnp.sum(every, axis=0)
    prefix = state + before
    carried = jnp.einsum("ihd,hde->ihe", queries.astype(F32), prefix, precision=highest)
    scores = jnp.einsum("ihd,jhd->hij", queries, key_rows, preferred_element_type=F32)
    causal = lax.broadcasted_iota(jnp.int32, (rows, rows), 0) >= lax.broadcasted_iota(
        jnp.int32, (rows, rows), 1
    )
    weights = jnp.where(causal[None], scores, 0.0).astype(BF16)
    local = jnp.einsum("hij,jhe->ihe", weights, value_rows, preferred_element_type=F32)
    attended = carried + local
    scaled = attended * lax.rsqrt(jnp.mean(attended * attended, axis=-1, keepdims=True) + 1e-06)
    head_out = (scaled.reshape(rows, width) * head_gain).astype(BF16)
    result = (wide + jnp.dot(head_out, out_full, preferred_element_type=F32)).astype(BF16)
    return (result, state + total)


def gathered_body(
    section_inputs, fresh_group, resident_state, qkv_weight, out_weight, input_gain, head_gain
):
    qkv_full, out_full = (
        lax.all_gather(qkv_weight[0], "row", axis=0, tiled=True),
        lax.all_gather(out_weight[0], "row", axis=0, tiled=True),
    )
    first_out, first_state = layer(
        section_inputs[0], resident_state[0], qkv_full, out_full, input_gain[0], head_gain[0]
    )
    arrived = passed_along(first_out, "section", 1)
    second_in = jnp.where(lax.axis_index("section") == 0, fresh_group, arrived)
    second_out, second_state = layer(
        second_in, first_state, qkv_full, out_full, input_gain[0], head_gain[0]
    )
    return (second_out[None], second_state[None])


def to_row(value, offset):
    return lax.ppermute(value, "row", [(i, i ^ offset) for i in range(lax.axis_size("row"))])


def to_next(value, offset):
    sections, rows = lax.axis_size("section"), lax.axis_size("row")
    pairs = [
        (s * rows + r, (s + 1) % sections * rows + (r ^ offset))
        for s in range(sections)
        for r in range(rows)
    ]
    return lax.ppermute(value, ("section", "row"), pairs)


def spread(value):
    count, half = lax.axis_size("row"), value.shape[0] // 2
    near = {o: to_row(value, o) for o in range(1, count) if o & (o - 1) == 0}
    pieces = {0: (value,), **{o: (near[o],) for o in near}}
    for o in range(1, count):
        if o in near:
            continue
        low = o & -o
        if o - low in near:
            pieces[o] = (
                to_row(near[low][:half], o - low),
                to_row(near[o - low][half:], low),
            )
        else:
            pieces[o] = (to_row(value, o),)
    return tuple(pieces[o] for o in range(count))


def flat(pieces):
    return [piece for block in pieces for piece in block]


def regroup(refs, sizes):
    refs = list(refs)
    return [[refs.pop(0) for _ in range(size)] for size in sizes]


def norm_kernel(x_ref, gain_ref, out_ref):
    wide = x_ref[...].astype(F32)
    mean = jnp.mean(wide * wide, axis=-1, keepdims=True)
    out_ref[...] = (wide * lax.rsqrt(mean + 1e-05) * gain_ref[...]).astype(BF16)


def norm(x, gain):
    return pl.pallas_call(
        norm_kernel,
        out_shape=jax.ShapeDtypeStruct(x.shape, BF16),
        in_specs=[VMEM, VMEM],
        out_specs=VMEM,
        name="norm",
    )(x, gain)


def attend_kernel(sizes, first, me_ref, *refs):
    count = len(sizes)
    x_refs = regroup(refs[: sum(sizes)], sizes)
    refs = refs[sum(sizes) :]
    w_refs, refs = refs[:count], refs[count:]
    state_ref, gain_ref, refs = refs[0], refs[1], refs[2:]
    if not first:
        resident_ref, refs = refs[0], refs[1:]
    ho_refs, refs = refs[:count], refs[count:]
    new_state_ref, refs = refs[0], refs[1:]
    if not first:
        change_ref, refs = refs[0], refs[1:]
    x_all, w_all, ho_all = refs
    me = me_ref[0]
    block = ho_refs[0].shape[0]
    depth = w_refs[0].shape[0]
    own, size = new_state_ref.shape[0], new_state_ref.shape[1]
    cols = own * size
    for o in range(count):
        at = me ^ o
        row = pl.multiple_of(at * block, block)
        for piece in x_refs[o]:
            x_all[pl.ds(row, piece.shape[0]), :] = piece[...]
            row = pl.multiple_of(row + piece.shape[0], piece.shape[0])
        w_all[pl.ds(pl.multiple_of(at * depth, depth), depth), :] = w_refs[o][...]
    parts = []
    for c in range(3):
        part = jnp.dot(
            x_all[...], w_all[:, c * cols : (c + 1) * cols], preferred_element_type=F32
        )
        if c < 2:
            part = part / (1.0 + jnp.exp(-part))
        parts.append(part.astype(BF16))
    queries, keys, values = parts
    causal = lax.broadcasted_iota(jnp.int32, (block, block), 0) >= lax.broadcasted_iota(
        jnp.int32, (block, block), 1
    )
    gains = gain_ref[:, pl.ds(pl.multiple_of(me * cols, cols), cols)]
    for h in range(own):
        head = slice(h * size, (h + 1) * size)
        start = state_ref[me * own + h] if first else state_ref[h]
        prefix = start
        for b in range(count):
            rows = slice(b * block, (b + 1) * block)
            q, k, v = queries[rows, head], keys[rows, head], values[rows, head]
            high = prefix.astype(BF16)
            low = (prefix - high.astype(F32)).astype(BF16)
            scores = lax.dot_general(
                q, k, (((1,), (1,)), ((), ())), preferred_element_type=F32
            )
            weights = jnp.where(causal, scores, 0.0).astype(BF16)
            attended = (
                jnp.dot(q, high, preferred_element_type=F32)
                + jnp.dot(q, low, preferred_element_type=F32)
                + jnp.dot(weights, v, preferred_element_type=F32)
            )
            mean = jnp.mean(attended * attended, axis=-1, keepdims=True)
            scaled = attended * lax.rsqrt(mean + 1e-06) * gains[:, head]
            ho_all[b, :, head] = scaled.astype(BF16)
            prefix = prefix + lax.dot_general(
                k, v, (((0,), (0,)), ((), ())), preferred_element_type=F32
            )
        new_state_ref[h] = prefix
        if not first:
            change_ref[h] = (prefix - resident_ref[me * own + h]).astype(BF16)
    for o in range(count):
        ho_refs[o][...] = ho_all[me ^ o]


def attend(me, blocks, weights, state, head_gain, resident):
    first = resident is None
    count = len(blocks)
    sizes = tuple(len(block) for block in blocks)
    block, width = blocks[0][0].shape
    depth, cols3 = weights[0].shape
    size = state.shape[-1]
    own = cols3 // 3 // size
    rows = block * count
    ins = [me, *flat(blocks), *weights, state, head_gain] + ([] if first else [resident])
    outs = [jax.ShapeDtypeStruct((block, own * size), BF16)] * count
    outs += [jax.ShapeDtypeStruct((own, size, size), F32)]
    outs += [] if first else [jax.ShapeDtypeStruct((own, size, size), BF16)]
    result = pl.pallas_call(
        functools.partial(attend_kernel, sizes, first),
        out_shape=outs,
        in_specs=[SMEM] + [VMEM] * (len(ins) - 1),
        out_specs=[VMEM] * len(outs),
        scratch_shapes=[
            pltpu.VMEM((rows, width), BF16),
            pltpu.VMEM((depth * count, cols3), BF16),
            pltpu.VMEM((count, block, own * size), BF16),
        ],
        cost_estimate=pl.CostEstimate(
            flops=2 * rows * width * cols3, bytes_accessed=8 << 20, transcendentals=0
        ),
        name="attend_first" if first else "attend_second",
    )(*ins)
    return result[:count], result[count], None if first else result[count + 1]


def project(ho_refs, w_refs, sizes, columns):
    total = None
    for ho_ref, pieces in zip(ho_refs, regroup(w_refs, sizes)):
        row = 0
        for piece in pieces:
            term = jnp.dot(
                ho_ref[:, row : row + piece.shape[0]],
                piece[:, columns],
                preferred_element_type=F32,
            )
            total = term if total is None else total + term
            row += piece.shape[0]
    return total


def out_kernel(sizes, first, chunk, flag_ref, *refs):
    count = len(sizes)
    ho_refs, refs = refs[:count], refs[count:]
    w_refs, refs = refs[: sum(sizes)], refs[sum(sizes) :]
    x_ref, fresh_ref, refs = refs[0], refs[1], refs[2:]
    if first:
        gain_ref, out_ref, normed_ref = refs
    else:
        (out_ref,) = refs
    swap = flag_ref[0] == 1
    width = x_ref.shape[1]
    square = None
    for at in range(0, width, chunk):
        columns = slice(at, at + chunk)
        x = x_ref[:, columns]
        if not first:
            x = jnp.where(swap, fresh_ref[:, columns].astype(F32), x.astype(F32))
        out = (x.astype(F32) + project(ho_refs, w_refs, sizes, columns)).astype(BF16)
        out_ref[:, columns] = out
        if first:
            wide = jnp.where(swap, fresh_ref[:, columns].astype(F32), out.astype(F32))
            normed_ref[:, columns] = wide.astype(BF16)
            term = jnp.sum(wide * wide, axis=-1, keepdims=True)
            square = term if square is None else square + term
    if first:
        scale = lax.rsqrt(square / width + 1e-05)
        for at in range(0, width, chunk):
            columns = slice(at, at + chunk)
            wide = normed_ref[:, columns].astype(F32)
            normed_ref[:, columns] = (wide * scale * gain_ref[:, columns]).astype(BF16)


def output(flag, head_outs, weights, x, fresh, next_gain):
    first = next_gain is not None
    sizes = tuple(len(block) for block in weights)
    ins = [flag, *head_outs, *flat(weights), x, fresh] + ([next_gain] if first else [])
    shape = jax.ShapeDtypeStruct(x.shape, BF16)
    depth = sum(h.shape[1] for h in head_outs)
    return pl.pallas_call(
        functools.partial(out_kernel, sizes, first, x.shape[1] // 4),
        out_shape=(shape, shape) if first else shape,
        in_specs=[SMEM] + [VMEM] * (len(ins) - 1),
        out_specs=(VMEM, VMEM) if first else VMEM,
        cost_estimate=pl.CostEstimate(
            flops=2 * x.size * depth, bytes_accessed=6 << 20, transcendentals=0
        ),
        name="output_first" if first else "output_second",
    )(*ins)


def finish_kernel(me_ref, resident_ref, own_ref, *refs):
    change_refs, out_ref = refs[:-1], refs[-1]
    me, own = me_ref[0], own_ref.shape[0]
    for h in range(own):
        out_ref[me * own + h] = own_ref[h]
        for o, change_ref in enumerate(change_refs):
            at = (me ^ (o + 1)) * own + h
            out_ref[at] = resident_ref[at] + change_ref[h].astype(F32)


def finish(me, resident, own_state, changes):
    return pl.pallas_call(
        finish_kernel,
        out_shape=jax.ShapeDtypeStruct(resident.shape, F32),
        in_specs=[SMEM] + [VMEM] * (2 + len(changes)),
        out_specs=VMEM,
        name="finish",
    )(me, resident, own_state, *changes)


def spread_body(
    section_inputs, fresh_group, resident_state, qkv_weight, out_weight, input_gain, head_gain
):
    count = lax.axis_size("row")
    sections = lax.axis_size("section")
    row = lax.axis_index("row")
    section = lax.axis_index("section")
    me = row.astype(jnp.int32)[None]
    at_last = (section == sections - 1).astype(jnp.int32)[None]
    at_first = (section == 0).astype(jnp.int32)[None]
    x = section_inputs[0]
    resident = resident_state[0]
    depth, cols3 = qkv_weight.shape[1:]
    cols = cols3 // 3 // count

    blocks = spread(norm(x, input_gain))
    by_owner = qkv_weight[0].reshape(depth, 3, count, cols)
    pieces = [
        lax.dynamic_index_in_dim(by_owner, row ^ o, 2, keepdims=False).reshape(depth, 3 * cols)
        for o in range(count)
    ]
    weights = [pieces[0]] + [to_row(pieces[o], o) for o in range(1, count)]
    next_gain = lax.ppermute(
        input_gain, "section", [((s + 1) % sections, s) for s in range(sections)]
    )
    out_weights = spread(out_weight[0])

    head_outs, own_state, _ = attend(me, blocks, weights, resident, head_gain, None)
    head_outs = [head_outs[0]] + [to_row(head_outs[o], o) for o in range(1, count)]
    first_out, normed = output(at_last, head_outs, out_weights, x, fresh_group, next_gain)

    blocks = tuple((to_next(normed, o),) for o in range(count))
    arrived = passed_along(first_out, "section", 1)
    head_outs, own_state, change = attend(me, blocks, weights, own_state, head_gain, resident)
    head_outs = [head_outs[0]] + [to_row(head_outs[o], o) for o in range(1, count)]
    changes = [to_row(change, o) for o in range(1, count)]
    second_out = output(at_first, head_outs, out_weights, arrived, fresh_group, None)
    final_state = finish(me, resident, own_state, changes)
    return (second_out[None], final_state[None])


def solution(mesh):
    in_specs = (
        P("section", "row", None),
        P("row", None),
        P("section", None, None, None),
        P("section", "row", None),
        P("section", "row", None),
        P("section", None),
        P("section", None),
    )
    out_specs = (P("section", "row", None), P("section", None, None, None))

    def whole(*args):
        count = mesh.shape["row"]
        heads = args[2].shape[1]
        even = heads % count == 0 and count & (count - 1) == 0
        body = spread_body if even else gathered_body
        return jax.shard_map(
            body, mesh=mesh, in_specs=in_specs, out_specs=out_specs, check_vma=False
        )(*args)

    return whole
```

```python
import functools

import jax
import jax.numpy as jnp
from jax import lax
from jax.experimental import pallas as pl
from jax.experimental.pallas import tpu as pltpu
from jax.sharding import PartitionSpec as P


VMEM = pl.BlockSpec(memory_space=pltpu.VMEM)
SMEM = pl.BlockSpec(memory_space=pltpu.SMEM)
F32 = jnp.float32
BF16 = jnp.bfloat16


def passed_along(value, axis, by):
    peers = lax.axis_size(axis)
    pairs = [(i, i + by) for i in range(peers) if 0 <= i + by < peers]
    return lax.ppermute(value, axis, pairs)


def layer(inputs, state, qkv_full, out_full, input_gain, head_gain):
    rows = inputs.shape[0]
    heads = state.shape[0]
    head_size = state.shape[1]
    width = heads * head_size
    highest = lax.Precision.HIGHEST
    wide = inputs.astype(F32)
    normed = (
        wide * lax.rsqrt(jnp.mean(wide * wide, axis=-1, keepdims=True) + 1e-05) * input_gain
    ).astype(BF16)
    projected = jnp.dot(normed, qkv_full, preferred_element_type=F32)
    queries = jax.nn.silu(projected[:, :width]).astype(BF16).reshape(rows, heads, head_size)
    key_rows = (
        jax.nn.silu(projected[:, width : 2 * width]).astype(BF16).reshape(rows, heads, head_size)
    )
    value_rows = projected[:, 2 * width :].astype(BF16).reshape(rows, heads, head_size)
    own_state = jnp.einsum("jhd,jhe->hde", key_rows, value_rows, preferred_element_type=F32)
    every = lax.all_gather(own_state[None].astype(BF16), "row", axis=0, tiled=True).astype(F32)
    order = lax.iota(jnp.int32, every.shape[0])
    earlier = (order < lax.axis_index("row")).astype(F32)
    before = jnp.sum(every * earlier[:, None, None, None], axis=0)
    total = jnp.sum(every, axis=0)
    prefix = state + before
    carried = jnp.einsum("ihd,hde->ihe", queries.astype(F32), prefix, precision=highest)
    scores = jnp.einsum("ihd,jhd->hij", queries, key_rows, preferred_element_type=F32)
    causal = lax.broadcasted_iota(jnp.int32, (rows, rows), 0) >= lax.broadcasted_iota(
        jnp.int32, (rows, rows), 1
    )
    weights = jnp.where(causal[None], scores, 0.0).astype(BF16)
    local = jnp.einsum("hij,jhe->ihe", weights, value_rows, preferred_element_type=F32)
    attended = carried + local
    scaled = attended * lax.rsqrt(jnp.mean(attended * attended, axis=-1, keepdims=True) + 1e-06)
    head_out = (scaled.reshape(rows, width) * head_gain).astype(BF16)
    result = (wide + jnp.dot(head_out, out_full, preferred_element_type=F32)).astype(BF16)
    return (result, state + total)


def gathered_body(
    section_inputs, fresh_group, resident_state, qkv_weight, out_weight, input_gain, head_gain
):
    qkv_full, out_full = (
        lax.all_gather(qkv_weight[0], "row", axis=0, tiled=True),
        lax.all_gather(out_weight[0], "row", axis=0, tiled=True),
    )
    first_out, first_state = layer(
        section_inputs[0], resident_state[0], qkv_full, out_full, input_gain[0], head_gain[0]
    )
    arrived = passed_along(first_out, "section", 1)
    second_in = jnp.where(lax.axis_index("section") == 0, fresh_group, arrived)
    second_out, second_state = layer(
        second_in, first_state, qkv_full, out_full, input_gain[0], head_gain[0]
    )
    return (second_out[None], second_state[None])


def to_row(value, offset):
    return lax.ppermute(value, "row", [(i, i ^ offset) for i in range(lax.axis_size("row"))])


def to_next(value, offset):
    sections, rows = lax.axis_size("section"), lax.axis_size("row")
    pairs = [
        (s * rows + r, (s + 1) % sections * rows + (r ^ offset))
        for s in range(sections)
        for r in range(rows)
    ]
    return lax.ppermute(value, ("section", "row"), pairs)


def spread(value, move=to_row):
    count, half = lax.axis_size("row"), value.shape[0] // 2
    near = {o: move(value, o) for o in range(1, count) if o & (o - 1) == 0}
    pieces = {o: (near[o],) for o in near}
    pieces[0] = (value if move is to_row else move(value, 0),)
    for o in range(1, count):
        if o in near:
            continue
        low = o & -o
        if o - low in near:
            pieces[o] = (
                to_row(near[low][:half], o - low),
                to_row(near[o - low][half:], low),
            )
        else:
            pieces[o] = (move(value, o),)
    return tuple(pieces[o] for o in range(count))


def flat(pieces):
    return [piece for block in pieces for piece in block]


def regroup(refs, sizes):
    refs = list(refs)
    return [[refs.pop(0) for _ in range(size)] for size in sizes]


def limit(mebibytes):
    return pltpu.CompilerParams(vmem_limit_bytes=mebibytes << 20)


def cut_kernel(me_ref, w_ref, *out_refs):
    count = len(out_refs)
    cols = out_refs[0].shape[1] // 3
    for o, out_ref in enumerate(out_refs):
        for c in range(3):
            at = pl.multiple_of((c * count + (me_ref[0] ^ o)) * cols, cols)
            out_ref[:, c * cols : (c + 1) * cols] = w_ref[:, pl.ds(at, cols)]


def cut(me, weight, count):
    depth, cols3 = weight.shape
    step = depth // 4 if depth % 64 == 0 else depth
    return pl.pallas_call(
        cut_kernel,
        grid=(depth // step,),
        out_shape=[jax.ShapeDtypeStruct((depth, cols3 // count), BF16)] * count,
        in_specs=[SMEM, pl.BlockSpec((step, cols3), lambda i: (i, 0))],
        out_specs=[pl.BlockSpec((step, cols3 // count), lambda i: (i, 0))] * count,
        compiler_params=limit(12),
        name="cut",
    )(me, weight)


def attend_kernel(sizes, first, me_ref, *refs):
    count = len(sizes)
    x_refs = regroup(refs[: sum(sizes)], sizes)
    refs = refs[sum(sizes) :]
    w_refs, refs = refs[:count], refs[count:]
    state_ref, gain_ref, refs = refs[0], refs[1], refs[2:]
    if first:
        input_gain_ref, refs = refs[0], refs[1:]
    else:
        resident_ref, refs = refs[0], refs[1:]
    ho_refs, refs = refs[:count], refs[count:]
    new_state_ref, refs = refs[0], refs[1:]
    if not first:
        change_ref, refs = refs[0], refs[1:]
    x_all, w_all, ho_all = refs
    me = me_ref[0]
    block = ho_refs[0].shape[0]
    depth = w_refs[0].shape[0]
    own, size = new_state_ref.shape[0], new_state_ref.shape[1]
    cols = own * size
    for o in range(count):
        at = me ^ o
        row = pl.multiple_of(at * block, block)
        for piece in x_refs[o]:
            x = piece[...]
            if first:
                wide = x.astype(F32)
                mean = jnp.mean(wide * wide, axis=-1, keepdims=True)
                x = (wide * lax.rsqrt(mean + 1e-05) * input_gain_ref[...]).astype(BF16)
            x_all[pl.ds(row, piece.shape[0]), :] = x
            row = pl.multiple_of(row + piece.shape[0], piece.shape[0])
        w_all[pl.ds(pl.multiple_of(at * depth, depth), depth), :] = w_refs[o][...]
    parts = []
    for c in range(3):
        part = jnp.dot(
            x_all[...], w_all[:, c * cols : (c + 1) * cols], preferred_element_type=F32
        )
        if c < 2:
            part = part / (1.0 + jnp.exp(-part))
        parts.append(part.astype(BF16))
    queries, keys, values = parts
    causal = lax.broadcasted_iota(jnp.int32, (block, block), 0) >= lax.broadcasted_iota(
        jnp.int32, (block, block), 1
    )
    gains = gain_ref[:, pl.ds(pl.multiple_of(me * cols, cols), cols)]
    for h in range(own):
        head = slice(h * size, (h + 1) * size)
        start = state_ref[me * own + h] if first else state_ref[h]
        prefix = start
        for b in range(count):
            rows = slice(b * block, (b + 1) * block)
            q, k, v = queries[rows, head], keys[rows, head], values[rows, head]
            high = prefix.astype(BF16)
            low = (prefix - high.astype(F32)).astype(BF16)
            scores = lax.dot_general(
                q, k, (((1,), (1,)), ((), ())), preferred_element_type=F32
            )
            weights = jnp.where(causal, scores, 0.0).astype(BF16)
            attended = (
                jnp.dot(q, high, preferred_element_type=F32)
                + jnp.dot(q, low, preferred_element_type=F32)
                + jnp.dot(weights, v, preferred_element_type=F32)
            )
            mean = jnp.mean(attended * attended, axis=-1, keepdims=True)
            scaled = attended * lax.rsqrt(mean + 1e-06) * gains[:, head]
            ho_all[b, :, head] = scaled.astype(BF16)
            prefix = prefix + lax.dot_general(
                k, v, (((0,), (0,)), ((), ())), preferred_element_type=F32
            )
        new_state_ref[h] = prefix
        if not first:
            change_ref[h] = (prefix - resident_ref[me * own + h]).astype(BF16)
    for o in range(count):
        ho_refs[o][...] = ho_all[me ^ o]


def attend(me, blocks, weights, state, head_gain, input_gain=None, resident=None):
    first = resident is None
    count = len(blocks)
    sizes = tuple(len(block) for block in blocks)
    block, width = blocks[0][0].shape
    depth, cols3 = weights[0].shape
    size = state.shape[-1]
    own = cols3 // 3 // size
    rows = block * count
    ins = [me, *flat(blocks), *weights, state, head_gain, input_gain if first else resident]
    outs = [jax.ShapeDtypeStruct((block, own * size), BF16)] * count
    outs += [jax.ShapeDtypeStruct((own, size, size), F32)]
    outs += [] if first else [jax.ShapeDtypeStruct((own, size, size), BF16)]
    result = pl.pallas_call(
        functools.partial(attend_kernel, sizes, first),
        out_shape=outs,
        in_specs=[SMEM] + [VMEM] * (len(ins) - 1),
        out_specs=[VMEM] * len(outs),
        scratch_shapes=[
            pltpu.VMEM((rows, width), BF16),
            pltpu.VMEM((depth * count, cols3), BF16),
            pltpu.VMEM((count, block, own * size), BF16),
        ],
        cost_estimate=pl.CostEstimate(
            flops=2 * rows * width * cols3, bytes_accessed=8 << 20, transcendentals=0
        ),
        compiler_params=limit(30),
        name="attend_first" if first else "attend_second",
    )(*ins)
    return result[:count], result[count], None if first else result[count + 1]


def project(ho_refs, w_refs, sizes, columns):
    total = None
    for ho_ref, pieces in zip(ho_refs, regroup(w_refs, sizes)):
        row = 0
        for piece in pieces:
            term = jnp.dot(
                ho_ref[:, row : row + piece.shape[0]],
                piece[:, columns],
                preferred_element_type=F32,
            )
            total = term if total is None else total + term
            row += piece.shape[0]
    return total


def out_kernel(sizes, first, chunk, flag_ref, *refs):
    count = len(sizes)
    ho_refs, refs = refs[:count], refs[count:]
    w_refs, refs = refs[: sum(sizes)], refs[sum(sizes) :]
    x_ref, fresh_ref, refs = refs[0], refs[1], refs[2:]
    if first:
        gain_ref, out_ref, normed_ref = refs
    else:
        (out_ref,) = refs
    swap = flag_ref[0] == 1
    width = x_ref.shape[1]
    square = None
    for at in range(0, width, chunk):
        columns = slice(at, at + chunk)
        x = x_ref[:, columns]
        if not first:
            x = jnp.where(swap, fresh_ref[:, columns].astype(F32), x.astype(F32))
        out = (x.astype(F32) + project(ho_refs, w_refs, sizes, columns)).astype(BF16)
        out_ref[:, columns] = out
        if first:
            wide = jnp.where(swap, fresh_ref[:, columns].astype(F32), out.astype(F32))
            normed_ref[:, columns] = wide.astype(BF16)
            term = jnp.sum(wide * wide, axis=-1, keepdims=True)
            square = term if square is None else square + term
    if first:
        scale = lax.rsqrt(square / width + 1e-05)
        for at in range(0, width, chunk):
            columns = slice(at, at + chunk)
            wide = normed_ref[:, columns].astype(F32)
            normed_ref[:, columns] = (wide * scale * gain_ref[:, columns]).astype(BF16)


def output(flag, head_outs, weights, x, fresh, next_gain):
    first = next_gain is not None
    sizes = tuple(len(block) for block in weights)
    ins = [flag, *head_outs, *flat(weights), x, fresh] + ([next_gain] if first else [])
    shape = jax.ShapeDtypeStruct(x.shape, BF16)
    depth = sum(h.shape[1] for h in head_outs)
    return pl.pallas_call(
        functools.partial(out_kernel, sizes, first, x.shape[1] // 4),
        out_shape=(shape, shape) if first else shape,
        in_specs=[SMEM] + [VMEM] * (len(ins) - 1),
        out_specs=(VMEM, VMEM) if first else VMEM,
        cost_estimate=pl.CostEstimate(
            flops=2 * x.size * depth, bytes_accessed=6 << 20, transcendentals=0
        ),
        compiler_params=limit(20),
        name="output_first" if first else "output_second",
    )(*ins)


def finish_kernel(me_ref, resident_ref, own_ref, *refs):
    change_refs, out_ref = refs[:-1], refs[-1]
    me, own = me_ref[0], own_ref.shape[0]
    for h in range(own):
        out_ref[me * own + h] = own_ref[h]
        for o, change_ref in enumerate(change_refs):
            at = (me ^ (o + 1)) * own + h
            out_ref[at] = resident_ref[at] + change_ref[h].astype(F32)


def finish(me, resident, own_state, changes):
    return pl.pallas_call(
        finish_kernel,
        out_shape=jax.ShapeDtypeStruct(resident.shape, F32),
        in_specs=[SMEM] + [VMEM] * (2 + len(changes)),
        out_specs=VMEM,
        compiler_params=limit(8),
        name="finish",
    )(me, resident, own_state, *changes)


def spread_body(
    section_inputs, fresh_group, resident_state, qkv_weight, out_weight, input_gain, head_gain
):
    count = lax.axis_size("row")
    sections = lax.axis_size("section")
    row = lax.axis_index("row")
    section = lax.axis_index("section")
    me = row.astype(jnp.int32)[None]
    at_last = (section == sections - 1).astype(jnp.int32)[None]
    at_first = (section == 0).astype(jnp.int32)[None]
    x = section_inputs[0]
    resident = resident_state[0]

    blocks = spread(x)
    next_gain = lax.ppermute(
        input_gain, "section", [((s + 1) % sections, s) for s in range(sections)]
    )
    pieces = cut(me, qkv_weight[0], count)
    weights = [pieces[0]] + [to_row(pieces[o], o) for o in range(1, count)]
    out_weights = spread(out_weight[0])

    head_outs, own_state, _ = attend(
        me, blocks, weights, resident, head_gain, input_gain=input_gain
    )
    head_outs = [head_outs[0]] + [to_row(head_outs[o], o) for o in range(1, count)]
    first_out, normed = output(at_last, head_outs, out_weights, x, fresh_group, next_gain)

    blocks = spread(normed, to_next)
    arrived = passed_along(first_out, "section", 1)
    head_outs, own_state, change = attend(
        me, blocks, weights, own_state, head_gain, resident=resident
    )
    head_outs = [head_outs[0]] + [to_row(head_outs[o], o) for o in range(1, count)]
    changes = [to_row(change, o) for o in range(1, count)]
    second_out = output(at_first, head_outs, out_weights, arrived, fresh_group, None)
    final_state = finish(me, resident, own_state, changes)
    return (second_out[None], final_state[None])


def solution(mesh):
    in_specs = (
        P("section", "row", None),
        P("row", None),
        P("section", None, None, None),
        P("section", "row", None),
        P("section", "row", None),
        P("section", None),
        P("section", None),
    )
    out_specs = (P("section", "row", None), P("section", None, None, None))

    def whole(*args):
        count = mesh.shape["row"]
        heads = args[2].shape[1]
        even = heads % count == 0 and count & (count - 1) == 0
        body = spread_body if even else gathered_body
        return jax.shard_map(
            body, mesh=mesh, in_specs=in_specs, out_specs=out_specs, check_vma=False
        )(*args)

    return whole
```

```python
import functools

import jax
import jax.numpy as jnp
from jax import lax
from jax.experimental import pallas as pl
from jax.experimental.pallas import tpu as pltpu
from jax.sharding import PartitionSpec as P


VMEM = pl.BlockSpec(memory_space=pltpu.VMEM)
SMEM = pl.BlockSpec(memory_space=pltpu.SMEM)
F32 = jnp.float32
BF16 = jnp.bfloat16


def passed_along(value, axis, by):
    peers = lax.axis_size(axis)
    pairs = [(i, i + by) for i in range(peers) if 0 <= i + by < peers]
    return lax.ppermute(value, axis, pairs)


def layer(inputs, state, qkv_full, out_full, input_gain, head_gain):
    rows = inputs.shape[0]
    heads = state.shape[0]
    head_size = state.shape[1]
    width = heads * head_size
    highest = lax.Precision.HIGHEST
    wide = inputs.astype(F32)
    normed = (
        wide * lax.rsqrt(jnp.mean(wide * wide, axis=-1, keepdims=True) + 1e-05) * input_gain
    ).astype(BF16)
    projected = jnp.dot(normed, qkv_full, preferred_element_type=F32)
    queries = jax.nn.silu(projected[:, :width]).astype(BF16).reshape(rows, heads, head_size)
    key_rows = (
        jax.nn.silu(projected[:, width : 2 * width]).astype(BF16).reshape(rows, heads, head_size)
    )
    value_rows = projected[:, 2 * width :].astype(BF16).reshape(rows, heads, head_size)
    own_state = jnp.einsum("jhd,jhe->hde", key_rows, value_rows, preferred_element_type=F32)
    every = lax.all_gather(own_state[None].astype(BF16), "row", axis=0, tiled=True).astype(F32)
    order = lax.iota(jnp.int32, every.shape[0])
    earlier = (order < lax.axis_index("row")).astype(F32)
    before = jnp.sum(every * earlier[:, None, None, None], axis=0)
    total = jnp.sum(every, axis=0)
    prefix = state + before
    carried = jnp.einsum("ihd,hde->ihe", queries.astype(F32), prefix, precision=highest)
    scores = jnp.einsum("ihd,jhd->hij", queries, key_rows, preferred_element_type=F32)
    causal = lax.broadcasted_iota(jnp.int32, (rows, rows), 0) >= lax.broadcasted_iota(
        jnp.int32, (rows, rows), 1
    )
    weights = jnp.where(causal[None], scores, 0.0).astype(BF16)
    local = jnp.einsum("hij,jhe->ihe", weights, value_rows, preferred_element_type=F32)
    attended = carried + local
    scaled = attended * lax.rsqrt(jnp.mean(attended * attended, axis=-1, keepdims=True) + 1e-06)
    head_out = (scaled.reshape(rows, width) * head_gain).astype(BF16)
    result = (wide + jnp.dot(head_out, out_full, preferred_element_type=F32)).astype(BF16)
    return (result, state + total)


def gathered_body(
    section_inputs, fresh_group, resident_state, qkv_weight, out_weight, input_gain, head_gain
):
    qkv_full, out_full = (
        lax.all_gather(qkv_weight[0], "row", axis=0, tiled=True),
        lax.all_gather(out_weight[0], "row", axis=0, tiled=True),
    )
    first_out, first_state = layer(
        section_inputs[0], resident_state[0], qkv_full, out_full, input_gain[0], head_gain[0]
    )
    arrived = passed_along(first_out, "section", 1)
    second_in = jnp.where(lax.axis_index("section") == 0, fresh_group, arrived)
    second_out, second_state = layer(
        second_in, first_state, qkv_full, out_full, input_gain[0], head_gain[0]
    )
    return (second_out[None], second_state[None])


def steps(section):
    return (1, 2) if section % 2 == 0 else (2, 1)


def along(value, axis, only=None):
    sections, rows = lax.axis_size("section"), lax.axis_size("row")
    pairs = [
        (s * rows + r, s * rows + (r ^ steps(s)[axis]))
        for s in range(sections)
        for r in range(rows)
        if only is None or s == only
    ]
    return lax.ppermute(value, ("section", "row"), pairs)


def to_next(value, over_a, over_b):
    sections, rows = lax.axis_size("section"), lax.axis_size("row")
    pairs = []
    for s in range(sections):
        to = (s + 1) % sections
        a, b = steps(to)
        pairs += [(s * rows + r, to * rows + (r ^ (a * over_a) ^ (b * over_b))) for r in range(rows)]
    return lax.ppermute(value, ("section", "row"), pairs)


def limit(mebibytes):
    return pltpu.CompilerParams(vmem_limit_bytes=mebibytes << 20)


def whereabouts(info_ref, count):
    info = info_ref[0]
    odd = info // (3 * count)
    return info % count, info // count % 3, 1 + odd, 2 - odd


def halve_kernel(count, info_ref, *refs):
    me, _, bit_a, bit_b = whereabouts(info_ref, count)
    sources, outs = refs[: len(refs) // 3], refs[len(refs) // 3 :]
    for i, source in enumerate(sources):
        depth = source.shape[1] // count
        for out_ref, low in zip(outs[2 * i :], (me & bit_b, (me & bit_b) ^ bit_b)):
            for part, block in enumerate((low, low | bit_a)):
                at = pl.multiple_of(block * depth, depth)
                out_ref[:, part * depth : (part + 1) * depth] = source[:, pl.ds(at, depth)]


def halve(info, count, *arrays):
    outs = [
        jax.ShapeDtypeStruct((x.shape[0], x.shape[1] // 2), x.dtype)
        for x in arrays
        for _ in range(2)
    ]
    return pl.pallas_call(
        functools.partial(halve_kernel, count),
        out_shape=outs,
        in_specs=[SMEM] + [VMEM] * len(arrays),
        out_specs=[VMEM] * len(outs),
        compiler_params=limit(6),
        name="halve",
    )(info, *arrays)


def cut_kernel(count, info_ref, w_ref, *out_refs):
    me, _, bit_a, bit_b = whereabouts(info_ref, count)
    cols = out_refs[0].shape[1] // 3
    for out_ref, offset in zip(out_refs, (0, bit_a, bit_b, bit_a | bit_b)):
        for c in range(3):
            at = pl.multiple_of((c * count + (me ^ offset)) * cols, cols)
            out_ref[:, c * cols : (c + 1) * cols] = w_ref[:, pl.ds(at, cols)]


def cut(info, weight, count):
    depth, cols3 = weight.shape
    return pl.pallas_call(
        functools.partial(cut_kernel, count),
        out_shape=[jax.ShapeDtypeStruct((depth, cols3 // count), BF16)] * 4,
        in_specs=[SMEM, VMEM],
        out_specs=[VMEM] * 4,
        compiler_params=limit(9),
        name="cut",
    )(info, weight)


def assemble(me, bit_a, bit_b, x_refs, x_all):
    offsets = (0, bit_a, bit_b, bit_a | bit_b)
    rows, width = x_refs[0].shape
    if width == x_all.shape[1]:
        for x_ref, offset in zip(x_refs, offsets):
            x_all[pl.ds(pl.multiple_of((me ^ offset) * rows, rows), rows), :] = x_ref[...]
        return
    block = rows // 2
    for j, x_ref in enumerate(x_refs):
        part = (me & bit_a) // bit_a
        columns = pl.ds(pl.multiple_of((part if j % 2 == 0 else 1 - part) * width, width), width)
        low = me & bit_b if j < 2 else (me & bit_b) ^ bit_b
        for t in range(2):
            at = pl.multiple_of((low | (t * bit_a)) * block, block)
            x_all[pl.ds(at, block), columns] = x_ref[t * block : (t + 1) * block, :]


def pair_weights(me, bit_a, w_refs, w_all):
    depth = w_refs[0].shape[0]
    second = (me & bit_a) // bit_a
    w_all[pl.ds(pl.multiple_of(second * depth, depth), depth), :] = w_refs[0][...]
    w_all[pl.ds(pl.multiple_of((1 - second) * depth, depth), depth), :] = w_refs[1][...]


def given_kernel(count, first, info_ref, gain_ref, *refs):
    me, _, bit_a, bit_b = whereabouts(info_ref, count)
    x_refs, refs = refs[:4], refs[4:]
    w_refs, refs = refs[: 1 + first], refs[1 + first :]
    out_ref, scaled_ref, x_all, refs = *refs[:3], refs[3:]
    w_all = refs[0] if first else w_refs[0]
    assemble(me, bit_a, bit_b, x_refs, x_all)
    if first:
        pair_weights(me, bit_a, w_refs, w_all)
    depth = scaled_ref.shape[1] // 2
    rows, tail = x_all.shape[0], out_ref.shape[0] - x_all.shape[0]
    total = None
    for part in range(2):
        at = pl.multiple_of(((me & bit_b) | (part * bit_a)) * depth, depth)
        columns = slice(part * depth, (part + 1) * depth)
        wide = x_all[:, columns].astype(F32)
        scaled_ref[:, columns] = (wide * gain_ref[:, pl.ds(at, depth)]).astype(BF16)
        term = lax.dot_general(
            jnp.ones((tail, depth), BF16),
            (wide * wide).astype(BF16),
            (((1,), (1,)), ((), ())),
            preferred_element_type=F32,
        )
        total = term if total is None else total + term
    out_ref[:rows, :] = jnp.dot(
        scaled_ref[...], w_all[...], preferred_element_type=F32
    ).astype(BF16)
    high = total.astype(BF16).astype(F32)
    line = lax.broadcasted_iota(jnp.int32, total.shape, 0)
    pair = jnp.where(line == 0, high, jnp.where(line == 1, total - high, 0.0))
    out_ref[rows:, :] = jnp.zeros((tail, out_ref.shape[1]), BF16)
    out_ref[rows:, :rows] = pair.astype(BF16)


def given_product(info, count, gain, x, w):
    first = len(w) > 1
    rows, half = x[0].size * len(x) * 2 // gain.shape[1], gain.shape[1] // 2
    cols = w[0].shape[1]
    outs = [jax.ShapeDtypeStruct((rows + 16, cols), BF16)]
    outs += [jax.ShapeDtypeStruct((rows, half), BF16)] * 2
    outs += [jax.ShapeDtypeStruct((half, cols), BF16)] if first else []
    return pl.pallas_call(
        functools.partial(given_kernel, count, first),
        out_shape=outs,
        in_specs=[SMEM] + [VMEM] * (1 + len(x) + len(w)),
        out_specs=[VMEM] * len(outs),
        cost_estimate=pl.CostEstimate(
            flops=2 * rows * half * cols, bytes_accessed=4 << 20, transcendentals=0
        ),
        compiler_params=limit(12),
        name="given_first" if first else "given_second",
    )(info, gain, *x, *w)


def own_kernel(count, first, info_ref, scaled_ref, *refs):
    me, _, bit_a, _ = whereabouts(info_ref, count)
    w_refs, refs = refs[: 1 + first], refs[1 + first :]
    out_ref = refs[0]
    w_all = refs[1] if first else w_refs[0]
    if first:
        pair_weights(me, bit_a, w_refs, w_all)
    out_ref[...] = jnp.dot(scaled_ref[...], w_all[...], preferred_element_type=F32)


def own_product(info, count, scaled, w):
    first = len(w) > 1
    rows, half = scaled.shape
    cols = w[0].shape[1]
    outs = [jax.ShapeDtypeStruct((rows, cols), F32)]
    outs += [jax.ShapeDtypeStruct((half, cols), BF16)] if first else []
    return pl.pallas_call(
        functools.partial(own_kernel, count, first),
        out_shape=outs,
        in_specs=[SMEM] + [VMEM] * (1 + len(w)),
        out_specs=[VMEM] * len(outs),
        cost_estimate=pl.CostEstimate(
            flops=2 * rows * half * cols, bytes_accessed=4 << 20, transcendentals=0
        ),
        compiler_params=limit(12),
        name="own_first" if first else "own_second",
    )(info, scaled, *w)


def attend_kernel(count, first, width, info_ref, *refs):
    own_ref, given_ref, got_ref, state_ref, gain_ref, refs = *refs[:5], refs[5:]
    if not first:
        resident_ref, refs = refs[0], refs[1:]
    ho_ref, new_state_ref, qkv = refs
    me, _, _, _ = whereabouts(info_ref, count)
    own, size = new_state_ref.shape[0], new_state_ref.shape[1]
    cols = own * size
    block = own_ref.shape[0] // count
    rows, square = own_ref.shape[0], None
    for ref in (given_ref, got_ref):
        tail = ref[rows:, :rows]
        term = lax.dot_general(
            tail,
            jnp.ones((tail.shape[0], 128), BF16),
            (((0,), (0,)), ((), ())),
            preferred_element_type=F32,
        )
        square = term if square is None else square + term
    scale = lax.rsqrt(square[:, :1] / width + 1e-05)
    for c in range(3):
        columns = slice(c * cols, (c + 1) * cols)
        part = (own_ref[:, columns] + got_ref[:rows, columns].astype(F32)) * scale
        if c < 2:
            part = part / (1.0 + jnp.exp(-part))
        qkv[:, columns] = part.astype(BF16)
    causal = lax.broadcasted_iota(jnp.int32, (block, block), 0) >= lax.broadcasted_iota(
        jnp.int32, (block, block), 1
    )
    gains = gain_ref[:, pl.ds(pl.multiple_of(me * cols, cols), cols)]
    for h in range(own):
        prefix = state_ref[me * own + h] if first else state_ref[h]
        for b in range(count):
            rows = slice(b * block, (b + 1) * block)
            q, k, v = (
                qkv[rows, c * cols + h * size : c * cols + (h + 1) * size] for c in range(3)
            )
            high = prefix.astype(BF16)
            low = (prefix - high.astype(F32)).astype(BF16)
            scores = lax.dot_general(
                q, k, (((1,), (1,)), ((), ())), preferred_element_type=F32
            )
            weights = jnp.where(causal, scores, 0.0).astype(BF16)
            attended = (
                jnp.dot(q, high, preferred_element_type=F32)
                + jnp.dot(q, low, preferred_element_type=F32)
                + jnp.dot(weights, v, preferred_element_type=F32)
            )
            mean = jnp.mean(attended * attended, axis=-1, keepdims=True)
            scaled = attended * lax.rsqrt(mean + 1e-06) * gains[:, h * size : (h + 1) * size]
            ho_ref[rows, h * size : (h + 1) * size] = scaled.astype(BF16)
            prefix = prefix + lax.dot_general(
                k, v, (((0,), (0,)), ((), ())), preferred_element_type=F32
            )
        new_state_ref[h] = prefix
        if not first:
            change = (prefix - resident_ref[me * own + h]).astype(BF16)
            ho_ref[count * block :, h * size : (h + 1) * size] = change


def attend(info, count, width, own, given, got, state, head_gain, resident=None):
    first = resident is None
    rows, cols3 = own.shape
    size = state.shape[-1]
    heads = cols3 // 3 // size
    ins = [info, own, given, got, state, head_gain] + ([] if first else [resident])
    outs = [
        jax.ShapeDtypeStruct((rows + (0 if first else size), heads * size), BF16),
        jax.ShapeDtypeStruct((heads, size, size), F32),
    ]
    return pl.pallas_call(
        functools.partial(attend_kernel, count, first, width),
        out_shape=outs,
        in_specs=[SMEM] + [VMEM] * (len(ins) - 1),
        out_specs=[VMEM] * len(outs),
        scratch_shapes=[pltpu.VMEM((rows, cols3), BF16)],
        cost_estimate=pl.CostEstimate(
            flops=10 * rows * heads * size * size, bytes_accessed=8 << 20, transcendentals=0
        ),
        compiler_params=limit(15),
        name="attend_first" if first else "attend_second",
    )(*ins)


def outgoing_kernel(count, mine, info_ref, *refs):
    ho_refs, w_refs, out_ref, lhs = refs[:2], refs[2:4], refs[4], refs[5]
    me, _, bit_a, bit_b = whereabouts(info_ref, count)
    low = me & bit_a if mine else (me & bit_a) ^ bit_a
    block, depth = ho_refs[0].shape[0] // count, ho_refs[0].shape[1]
    for t in range(2):
        at = pl.multiple_of((low | (t * bit_b)) * block, block)
        for i, ho_ref in enumerate(ho_refs):
            lhs[t * block : (t + 1) * block, i * depth : (i + 1) * depth] = ho_ref[
                pl.ds(at, block), :
            ]
    total = None
    for i, w_ref in enumerate(w_refs):
        term = jnp.dot(
            lhs[:, i * depth : (i + 1) * depth], w_ref[...], preferred_element_type=F32
        )
        total = term if total is None else total + term
    out_ref[...] = total.astype(out_ref.dtype)


def outgoing(info, count, heads, weights, mine):
    rows, depth = heads[0].shape[0] // 2, heads[0].shape[1]
    cols = weights[0].shape[1]
    return pl.pallas_call(
        functools.partial(outgoing_kernel, count, mine),
        out_shape=jax.ShapeDtypeStruct((rows, cols), F32 if mine else BF16),
        in_specs=[SMEM] + [VMEM] * 4,
        out_specs=VMEM,
        scratch_shapes=[pltpu.VMEM((rows, 2 * depth), BF16)],
        cost_estimate=pl.CostEstimate(
            flops=4 * rows * depth * cols, bytes_accessed=4 << 20, transcendentals=0
        ),
        compiler_params=limit(9),
        name="outgoing_mine" if mine else "outgoing_given",
    )(info, *heads, *weights)


def quarter_kernel(count, info_ref, own_ref, got_ref, x_ref, fresh_ref, partner_ref, *refs):
    next_mine, next_other, quarter = refs
    me, place, bit_a, bit_b = whereabouts(info_ref, count)
    block, depth = fresh_ref.shape[0], own_ref.shape[1] // 2
    second = (me & bit_b) // bit_b
    here = pl.ds(pl.multiple_of(second * block, block), block)
    there = pl.ds(pl.multiple_of((1 - second) * block, block), block)
    for t in range(2):
        rows = slice(t * block, (t + 1) * block)
        at = pl.multiple_of(((me & bit_a) | (t * bit_b)) * block, block)
        x = x_ref[pl.ds(at, block), :].astype(F32)
        quarter[rows, :] = (x + own_ref[rows, :] + got_ref[rows, :].astype(F32)).astype(BF16)

    @pl.when(place == 1)
    def _():
        quarter[here, :] = fresh_ref[...]
        quarter[there, :] = partner_ref[...]

    part = (me & bit_a) // bit_a
    next_mine[...] = quarter[:, pl.ds(pl.multiple_of(part * depth, depth), depth)]
    next_other[...] = quarter[:, pl.ds(pl.multiple_of((1 - part) * depth, depth), depth)]


def quarter(info, count, own, got, x, fresh, fresh_partner):
    rows, cols = own.shape
    block = jax.ShapeDtypeStruct((rows, cols // 2), BF16)
    return pl.pallas_call(
        functools.partial(quarter_kernel, count),
        out_shape=(block, block),
        in_specs=[SMEM] + [VMEM] * 5,
        out_specs=(VMEM, VMEM),
        scratch_shapes=[pltpu.VMEM((rows, cols), BF16)],
        cost_estimate=pl.CostEstimate(
            flops=4 * rows * cols, bytes_accessed=4 << 20, transcendentals=0
        ),
        compiler_params=limit(9),
        name="quarter",
    )(info, own, got, x, fresh, fresh_partner)


def deal_kernel(count, info_ref, *refs):
    ho_refs, w_refs, x_ref, refs = refs[:2], refs[2:4], refs[4], refs[5:]
    keep_ref, a_ref, b_ref, cross_ref, product = refs
    me, _, bit_a, bit_b = whereabouts(info_ref, count)
    rows, block = x_ref.shape[0], keep_ref.shape[0]
    total = None
    for ho_ref, w_ref in zip(ho_refs, w_refs):
        term = jnp.dot(ho_ref[:rows, :], w_ref[...], preferred_element_type=F32)
        total = term if total is None else total + term
    product[...] = total
    for out_ref, offset, residual in (
        (cross_ref, bit_a | bit_b, False),
        (a_ref, bit_a, False),
        (b_ref, bit_b, True),
        (keep_ref, 0, True),
    ):
        at = pl.ds(pl.multiple_of((me ^ offset) * block, block), block)
        out = product[at, :]
        if residual:
            out = out + x_ref[at, :].astype(F32)
        out_ref[:block, :] = out.astype(out_ref.dtype)
    size, cols = ho_refs[0].shape[0] - rows, ho_refs[0].shape[1]
    fold = x_ref.shape[1] // cols
    high = size // fold
    for i, ho_ref in enumerate(ho_refs):
        for q in range(fold):
            a_ref[block + i * high : block + (i + 1) * high, q * cols : (q + 1) * cols] = ho_ref[
                rows + q * high : rows + (q + 1) * high, :
            ]


def deal(info, count, heads, weights, x):
    rows, cols = x.shape
    block = rows // count
    size = heads[0].shape[0] - rows
    part = jax.ShapeDtypeStruct((block, cols), BF16)
    wide = jax.ShapeDtypeStruct((block, cols), F32)
    more = jax.ShapeDtypeStruct((block + 2 * size * heads[0].shape[1] // cols, cols), BF16)
    return pl.pallas_call(
        functools.partial(deal_kernel, count),
        out_shape=(wide, more, wide, part),
        in_specs=[SMEM] + [VMEM] * 5,
        out_specs=(VMEM,) * 4,
        scratch_shapes=[pltpu.VMEM((rows, cols), F32)],
        cost_estimate=pl.CostEstimate(
            flops=4 * rows * heads[0].shape[1] * cols, bytes_accessed=4 << 20, transcendentals=0
        ),
        compiler_params=limit(12),
        name="deal",
    )(info, *heads, *weights, x)


def combine_kernel(mine_ref, got_ref, out_ref):
    out_ref[...] = (mine_ref[...] + got_ref[...].astype(F32)).astype(BF16)


def combine(mine, got):
    return pl.pallas_call(
        combine_kernel,
        out_shape=jax.ShapeDtypeStruct(got.shape, BF16),
        in_specs=[VMEM, VMEM],
        out_specs=VMEM,
        compiler_params=limit(4),
        name="combine",
    )(mine, got)


def last_kernel(count, info_ref, keep_ref, a_ref, b_ref, heads_ref, *refs):
    resident_ref, own_ref, out_ref, final_ref = refs
    me, _, bit_a, bit_b = whereabouts(info_ref, count)
    block, width = out_ref.shape
    depth = width // count
    for t in range(2):
        columns = slice(t * depth, (t + 1) * depth)
        out = keep_ref[:, columns] + a_ref[:block, columns].astype(F32)
        for low, half in ((me & bit_b, out.astype(BF16)), ((me & bit_b) ^ bit_b, b_ref[:, columns])):
            at = pl.multiple_of((low | (t * bit_a)) * depth, depth)
            out_ref[:, pl.ds(at, depth)] = half
    own, size = own_ref.shape[0], own_ref.shape[1]
    cols = own * size
    fold = a_ref.shape[1] // cols
    high = size // fold
    rows = heads_ref.shape[0] - size
    for h in range(own):
        final_ref[me * own + h] = own_ref[h]
        columns = slice(h * size, (h + 1) * size)
        at = (me ^ bit_b) * own + h
        final_ref[at] = resident_ref[at] + heads_ref[rows:, columns].astype(F32)
        for i, offset in enumerate((bit_a, bit_a | bit_b)):
            at = (me ^ offset) * own + h
            for q in range(fold):
                inner = slice(q * high, (q + 1) * high)
                change = a_ref[
                    block + i * high : block + (i + 1) * high,
                    q * cols + h * size : q * cols + (h + 1) * size,
                ]
                final_ref[at, inner, :] = resident_ref[at, inner, :] + change.astype(F32)


def last(info, count, keep, from_a, from_b, heads_b, resident, own_state):
    block, half = keep.shape
    return pl.pallas_call(
        functools.partial(last_kernel, count),
        out_shape=(
            jax.ShapeDtypeStruct((block, 2 * half), BF16),
            jax.ShapeDtypeStruct(resident.shape, F32),
        ),
        in_specs=[SMEM] + [VMEM] * 6,
        out_specs=(VMEM, VMEM),
        cost_estimate=pl.CostEstimate(
            flops=4 * block * half, bytes_accessed=4 << 20, transcendentals=0
        ),
        compiler_params=limit(9),
        name="last",
    )(info, keep, from_a, from_b, heads_b, resident, own_state)


def paired_body(
    section_inputs, fresh_group, resident_state, qkv_weight, out_weight, input_gain, head_gain
):
    count = lax.axis_size("row")
    sections = lax.axis_size("section")
    row, section = lax.axis_index("row"), lax.axis_index("section")
    place = jnp.where(section == 0, 2, jnp.where(section == sections - 1, 1, 0))
    info = (row + count * (place + 3 * (section % 2))).astype(jnp.int32)[None]
    x, resident, width = section_inputs[0], resident_state[0], input_gain.shape[1]

    own_half, other_half = halve(info, count, x)
    from_b = along(other_half, 1)
    from_a = along(own_half, 0)
    mine, partner, mine_b, partner_b = cut(info, qkv_weight[0], count)
    partner_b = along(partner_b, 0)
    from_far = along(from_b, 0)
    partner = along(partner, 0)
    out_own, out_other, fresh_own, fresh_other = halve(
        info, count, out_weight[0], fresh_group
    )
    outs_b = along(out_other, 1)
    fresh_partner = along(fresh_other, 1, sections - 1)
    given, scaled, rows, columns_b = given_product(
        info,
        count,
        input_gain,
        [own_half, from_a, from_b, from_far],
        [mine_b, partner_b],
    )
    got = along(given, 1)
    own, columns = own_product(info, count, scaled, [mine, partner])
    heads, own_state = attend(
        info, count, width, own, given, got, resident, head_gain
    )
    heads_b = along(heads, 1)
    pair = ([heads, heads_b], [out_own, outs_b])
    given_out = outgoing(info, count, *pair, mine=False)
    got_out = along(given_out, 0)
    own_out = outgoing(info, count, *pair, mine=True)
    next_mine, next_other = quarter(info, count, own_out, got_out, rows, fresh_own, fresh_partner)
    from_b = to_next(next_other, 0, 1)
    from_a = to_next(next_mine, 1, 0)
    own_half = to_next(next_mine, 0, 0)
    from_far = along(from_b, 0)
    given, scaled, rows = given_product(
        info, count, input_gain, [own_half, from_a, from_b, from_far], [columns_b]
    )
    got = along(given, 1)
    (own,) = own_product(info, count, scaled, [columns])
    heads, own_state = attend(info, count, width, own, given, got, own_state, head_gain, resident)
    heads_b = along(heads, 1)
    keep, to_a, to_b, cross = deal(
        info, count, [heads, heads_b], [out_own, outs_b], rows
    )
    cross = along(cross, 0)
    from_a = along(to_a, 0)
    to_b = combine(to_b, cross)
    from_b = along(to_b, 1)
    second_out, final_state = last(info, count, keep, from_a, from_b, heads_b, resident, own_state)
    return (second_out[None], final_state[None])


def solution(mesh):
    in_specs = (
        P("section", "row", None),
        P("row", None),
        P("section", None, None, None),
        P("section", "row", None),
        P("section", "row", None),
        P("section", None),
        P("section", None),
    )
    out_specs = (P("section", "row", None), P("section", None, None, None))

    def whole(*args):
        count = mesh.shape["row"]
        heads, size = args[2].shape[1:3]
        block = args[0].shape[1] // count
        paired = count == 4 and mesh.shape["section"] % 2 == 0 and heads % count == 0
        paired = paired and block * count <= 3 * heads // count * size
        body = paired_body if paired else gathered_body
        return jax.shard_map(
            body, mesh=mesh, in_specs=in_specs, out_specs=out_specs, check_vma=False
        )(*args)

    return whole
```

```python
import functools

import jax
import jax.numpy as jnp
from jax import lax
from jax.experimental import pallas as pl
from jax.experimental.pallas import tpu as pltpu
from jax.sharding import PartitionSpec as P


VMEM = pl.BlockSpec(memory_space=pltpu.VMEM)
SMEM = pl.BlockSpec(memory_space=pltpu.SMEM)
F32 = jnp.float32
BF16 = jnp.bfloat16


def passed_along(value, axis, by):
    peers = lax.axis_size(axis)
    pairs = [(i, i + by) for i in range(peers) if 0 <= i + by < peers]
    return lax.ppermute(value, axis, pairs)


def layer(inputs, state, qkv_full, out_full, input_gain, head_gain):
    rows = inputs.shape[0]
    heads = state.shape[0]
    head_size = state.shape[1]
    width = heads * head_size
    highest = lax.Precision.HIGHEST
    wide = inputs.astype(F32)
    normed = (
        wide * lax.rsqrt(jnp.mean(wide * wide, axis=-1, keepdims=True) + 1e-05) * input_gain
    ).astype(BF16)
    projected = jnp.dot(normed, qkv_full, preferred_element_type=F32)
    queries = jax.nn.silu(projected[:, :width]).astype(BF16).reshape(rows, heads, head_size)
    key_rows = (
        jax.nn.silu(projected[:, width : 2 * width]).astype(BF16).reshape(rows, heads, head_size)
    )
    value_rows = projected[:, 2 * width :].astype(BF16).reshape(rows, heads, head_size)
    own_state = jnp.einsum("jhd,jhe->hde", key_rows, value_rows, preferred_element_type=F32)
    every = lax.all_gather(own_state[None].astype(BF16), "row", axis=0, tiled=True).astype(F32)
    order = lax.iota(jnp.int32, every.shape[0])
    earlier = (order < lax.axis_index("row")).astype(F32)
    before = jnp.sum(every * earlier[:, None, None, None], axis=0)
    total = jnp.sum(every, axis=0)
    prefix = state + before
    carried = jnp.einsum("ihd,hde->ihe", queries.astype(F32), prefix, precision=highest)
    scores = jnp.einsum("ihd,jhd->hij", queries, key_rows, preferred_element_type=F32)
    causal = lax.broadcasted_iota(jnp.int32, (rows, rows), 0) >= lax.broadcasted_iota(
        jnp.int32, (rows, rows), 1
    )
    weights = jnp.where(causal[None], scores, 0.0).astype(BF16)
    local = jnp.einsum("hij,jhe->ihe", weights, value_rows, preferred_element_type=F32)
    attended = carried + local
    scaled = attended * lax.rsqrt(jnp.mean(attended * attended, axis=-1, keepdims=True) + 1e-06)
    head_out = (scaled.reshape(rows, width) * head_gain).astype(BF16)
    result = (wide + jnp.dot(head_out, out_full, preferred_element_type=F32)).astype(BF16)
    return (result, state + total)


def gathered_body(
    section_inputs, fresh_group, resident_state, qkv_weight, out_weight, input_gain, head_gain
):
    qkv_full, out_full = (
        lax.all_gather(qkv_weight[0], "row", axis=0, tiled=True),
        lax.all_gather(out_weight[0], "row", axis=0, tiled=True),
    )
    first_out, first_state = layer(
        section_inputs[0], resident_state[0], qkv_full, out_full, input_gain[0], head_gain[0]
    )
    arrived = passed_along(first_out, "section", 1)
    second_in = jnp.where(lax.axis_index("section") == 0, fresh_group, arrived)
    second_out, second_state = layer(
        second_in, first_state, qkv_full, out_full, input_gain[0], head_gain[0]
    )
    return (second_out[None], second_state[None])


def steps(section):
    return (1, 2) if section % 2 == 0 else (2, 1)


def along(value, axis, only=None):
    sections, rows = lax.axis_size("section"), lax.axis_size("row")
    pairs = [
        (s * rows + r, s * rows + (r ^ steps(s)[axis]))
        for s in range(sections)
        for r in range(rows)
        if only is None or s == only
    ]
    return lax.ppermute(value, ("section", "row"), pairs)


def to_next(value, over_a, over_b):
    sections, rows = lax.axis_size("section"), lax.axis_size("row")
    pairs = []
    for s in range(sections):
        to = (s + 1) % sections
        a, b = steps(to)
        pairs += [(s * rows + r, to * rows + (r ^ (a * over_a) ^ (b * over_b))) for r in range(rows)]
    return lax.ppermute(value, ("section", "row"), pairs)


def limit(mebibytes):
    return pltpu.CompilerParams(vmem_limit_bytes=mebibytes << 20)


def whereabouts(info_ref, count):
    info = info_ref[0]
    odd = info // (3 * count)
    return info % count, info // count % 3, 1 + odd, 2 - odd


def halve_kernel(count, info_ref, *refs):
    me, _, bit_a, bit_b = whereabouts(info_ref, count)
    sources, outs = refs[: len(refs) // 3], refs[len(refs) // 3 :]
    for i, source in enumerate(sources):
        depth = source.shape[1] // count
        for out_ref, low in zip(outs[2 * i :], (me & bit_b, (me & bit_b) ^ bit_b)):
            for part, block in enumerate((low, low | bit_a)):
                at = pl.multiple_of(block * depth, depth)
                out_ref[:, part * depth : (part + 1) * depth] = source[:, pl.ds(at, depth)]


def halve(info, count, *arrays):
    outs = [
        jax.ShapeDtypeStruct((x.shape[0], x.shape[1] // 2), x.dtype)
        for x in arrays
        for _ in range(2)
    ]
    return pl.pallas_call(
        functools.partial(halve_kernel, count),
        out_shape=outs,
        in_specs=[SMEM] + [VMEM] * len(arrays),
        out_specs=[VMEM] * len(outs),
        compiler_params=limit(6),
        name="halve",
    )(info, *arrays)


def cut_kernel(count, info_ref, w_ref, *out_refs):
    me, _, bit_a, bit_b = whereabouts(info_ref, count)
    cols = out_refs[0].shape[1] // 3
    for out_ref, offset in zip(out_refs, (0, bit_a, bit_b, bit_a | bit_b)):
        for c in range(3):
            at = pl.multiple_of((c * count + (me ^ offset)) * cols, cols)
            out_ref[:, c * cols : (c + 1) * cols] = w_ref[:, pl.ds(at, cols)]


def cut(info, weight, count):
    depth, cols3 = weight.shape
    return pl.pallas_call(
        functools.partial(cut_kernel, count),
        out_shape=[jax.ShapeDtypeStruct((depth, cols3 // count), BF16)] * 4,
        in_specs=[SMEM, VMEM],
        out_specs=[VMEM] * 4,
        compiler_params=limit(9),
        name="cut",
    )(info, weight)


def assemble(me, bit_a, bit_b, x_refs, x_all):
    offsets = (0, bit_a, bit_b, bit_a | bit_b)
    rows, width = x_refs[0].shape
    if width == x_all.shape[1]:
        for x_ref, offset in zip(x_refs, offsets):
            x_all[pl.ds(pl.multiple_of((me ^ offset) * rows, rows), rows), :] = x_ref[...]
        return
    block = rows // 2
    for j, x_ref in enumerate(x_refs):
        part = (me & bit_a) // bit_a
        columns = pl.ds(pl.multiple_of((part if j % 2 == 0 else 1 - part) * width, width), width)
        low = me & bit_b if j < 2 else (me & bit_b) ^ bit_b
        for t in range(2):
            at = pl.multiple_of((low | (t * bit_a)) * block, block)
            x_all[pl.ds(at, block), columns] = x_ref[t * block : (t + 1) * block, :]


def pair_weights(me, bit_a, w_refs, w_all):
    depth = w_refs[0].shape[0]
    second = (me & bit_a) // bit_a
    w_all[pl.ds(pl.multiple_of(second * depth, depth), depth), :] = w_refs[0][...]
    w_all[pl.ds(pl.multiple_of((1 - second) * depth, depth), depth), :] = w_refs[1][...]


def given_kernel(count, first, info_ref, gain_ref, *refs):
    me, _, bit_a, bit_b = whereabouts(info_ref, count)
    x_refs, refs = refs[:4], refs[4:]
    w_refs, refs = refs[: 1 + first], refs[1 + first :]
    out_ref, scaled_ref, x_all, refs = *refs[:3], refs[3:]
    w_all = refs[0] if first else w_refs[0]
    assemble(me, bit_a, bit_b, x_refs, x_all)
    if first:
        pair_weights(me, bit_a, w_refs, w_all)
    depth = scaled_ref.shape[1] // 2
    rows, tail = x_all.shape[0], out_ref.shape[0] - x_all.shape[0]
    total = None
    for part in range(2):
        at = pl.multiple_of(((me & bit_b) | (part * bit_a)) * depth, depth)
        columns = slice(part * depth, (part + 1) * depth)
        wide = x_all[:, columns].astype(F32)
        scaled_ref[:, columns] = (wide * gain_ref[:, pl.ds(at, depth)]).astype(BF16)
        term = lax.dot_general(
            jnp.ones((tail, depth), BF16),
            (wide * wide).astype(BF16),
            (((1,), (1,)), ((), ())),
            preferred_element_type=F32,
        )
        total = term if total is None else total + term
    out_ref[:rows, :] = jnp.dot(
        scaled_ref[...], w_all[...], preferred_element_type=F32
    ).astype(BF16)
    high = total.astype(BF16).astype(F32)
    line = lax.broadcasted_iota(jnp.int32, total.shape, 0)
    pair = jnp.where(line == 0, high, jnp.where(line == 1, total - high, 0.0))
    out_ref[rows:, :] = jnp.zeros((tail, out_ref.shape[1]), BF16)
    out_ref[rows:, :rows] = pair.astype(BF16)


def given_product(info, count, gain, x, w):
    first = len(w) > 1
    rows, half = x[0].size * len(x) * 2 // gain.shape[1], gain.shape[1] // 2
    cols = w[0].shape[1]
    outs = [jax.ShapeDtypeStruct((rows + 16, cols), BF16)]
    outs += [jax.ShapeDtypeStruct((rows, half), BF16)] * 2
    outs += [jax.ShapeDtypeStruct((half, cols), BF16)] if first else []
    return pl.pallas_call(
        functools.partial(given_kernel, count, first),
        out_shape=outs,
        in_specs=[SMEM] + [VMEM] * (1 + len(x) + len(w)),
        out_specs=[VMEM] * len(outs),
        cost_estimate=pl.CostEstimate(
            flops=2 * rows * half * cols, bytes_accessed=4 << 20, transcendentals=0
        ),
        compiler_params=limit(12),
        name="given_first" if first else "given_second",
    )(info, gain, *x, *w)


def own_kernel(count, first, info_ref, scaled_ref, *refs):
    me, _, bit_a, _ = whereabouts(info_ref, count)
    w_refs, refs = refs[: 1 + first], refs[1 + first :]
    out_ref = refs[0]
    w_all = refs[1] if first else w_refs[0]
    if first:
        pair_weights(me, bit_a, w_refs, w_all)
    out_ref[...] = jnp.dot(scaled_ref[...], w_all[...], preferred_element_type=F32)


def own_product(info, count, scaled, w):
    first = len(w) > 1
    rows, half = scaled.shape
    cols = w[0].shape[1]
    outs = [jax.ShapeDtypeStruct((rows, cols), F32)]
    outs += [jax.ShapeDtypeStruct((half, cols), BF16)] if first else []
    return pl.pallas_call(
        functools.partial(own_kernel, count, first),
        out_shape=outs,
        in_specs=[SMEM] + [VMEM] * (1 + len(w)),
        out_specs=[VMEM] * len(outs),
        cost_estimate=pl.CostEstimate(
            flops=2 * rows * half * cols, bytes_accessed=4 << 20, transcendentals=0
        ),
        compiler_params=limit(12),
        name="own_first" if first else "own_second",
    )(info, scaled, *w)


def attend_kernel(count, first, width, info_ref, *refs):
    own_ref, given_ref, got_ref, state_ref, gain_ref, refs = *refs[:5], refs[5:]
    if not first:
        resident_ref, refs = refs[0], refs[1:]
    other_ref, mine_ref, new_state_ref, qkv, ho_all = refs
    me, _, bit_a, bit_b = whereabouts(info_ref, count)
    own, size = new_state_ref.shape[0], new_state_ref.shape[1]
    cols = own * size
    block = own_ref.shape[0] // count
    rows, square = own_ref.shape[0], None
    for ref in (given_ref, got_ref):
        tail = ref[rows:, :rows]
        term = lax.dot_general(
            tail,
            jnp.ones((tail.shape[0], 128), BF16),
            (((0,), (0,)), ((), ())),
            preferred_element_type=F32,
        )
        square = term if square is None else square + term
    scale = lax.rsqrt(square[:, :1] / width + 1e-05)
    for c in range(3):
        columns = slice(c * cols, (c + 1) * cols)
        part = (own_ref[:, columns] + got_ref[:rows, columns].astype(F32)) * scale
        if c < 2:
            part = part / (1.0 + jnp.exp(-part))
        qkv[:, columns] = part.astype(BF16)
    causal = lax.broadcasted_iota(jnp.int32, (block, block), 0) >= lax.broadcasted_iota(
        jnp.int32, (block, block), 1
    )
    gains = gain_ref[:, pl.ds(pl.multiple_of(me * cols, cols), cols)]
    for h in range(own):
        prefix = state_ref[me * own + h] if first else state_ref[h]
        for b in range(count):
            rows = slice(b * block, (b + 1) * block)
            q, k, v = (
                qkv[rows, c * cols + h * size : c * cols + (h + 1) * size] for c in range(3)
            )
            high = prefix.astype(BF16)
            low = (prefix - high.astype(F32)).astype(BF16)
            scores = lax.dot_general(
                q, k, (((1,), (1,)), ((), ())), preferred_element_type=F32
            )
            weights = jnp.where(causal, scores, 0.0).astype(BF16)
            attended = (
                jnp.dot(q, high, preferred_element_type=F32)
                + jnp.dot(q, low, preferred_element_type=F32)
                + jnp.dot(weights, v, preferred_element_type=F32)
            )
            mean = jnp.mean(attended * attended, axis=-1, keepdims=True)
            scaled = attended * lax.rsqrt(mean + 1e-06) * gains[:, h * size : (h + 1) * size]
            ho_all[rows, h * size : (h + 1) * size] = scaled.astype(BF16)
            prefix = prefix + lax.dot_general(
                k, v, (((0,), (0,)), ((), ())), preferred_element_type=F32
            )
        new_state_ref[h] = prefix
        if not first:
            change = (prefix - resident_ref[me * own + h]).astype(BF16)
            mine_ref[2 * block :, h * size : (h + 1) * size] = change
    for ref, low in ((other_ref, (me & bit_a) ^ bit_a), (mine_ref, me & bit_a)):
        for t in range(2):
            at = pl.multiple_of((low | (t * bit_b)) * block, block)
            ref[t * block : (t + 1) * block, :] = ho_all[pl.ds(at, block), :]


def attend(info, count, width, own, given, got, state, head_gain, resident=None):
    first = resident is None
    rows, cols3 = own.shape
    size = state.shape[-1]
    heads = cols3 // 3 // size
    ins = [info, own, given, got, state, head_gain] + ([] if first else [resident])
    outs = [
        jax.ShapeDtypeStruct((rows // 2, heads * size), BF16),
        jax.ShapeDtypeStruct((rows // 2 + (0 if first else size), heads * size), BF16),
        jax.ShapeDtypeStruct((heads, size, size), F32),
    ]
    return pl.pallas_call(
        functools.partial(attend_kernel, count, first, width),
        out_shape=outs,
        in_specs=[SMEM] + [VMEM] * (len(ins) - 1),
        out_specs=[VMEM] * len(outs),
        scratch_shapes=[
            pltpu.VMEM((rows, cols3), BF16),
            pltpu.VMEM((rows, heads * size), BF16),
        ],
        cost_estimate=pl.CostEstimate(
            flops=10 * rows * heads * size * size, bytes_accessed=8 << 20, transcendentals=0
        ),
        compiler_params=limit(15),
        name="attend_first" if first else "attend_second",
    )(*ins)


def product_of(ho_refs, w_refs, rows):
    total = None
    for ho_ref, w_ref in zip(ho_refs, w_refs):
        term = jnp.dot(ho_ref[rows, :], w_ref[...], preferred_element_type=F32)
        total = term if total is None else total + term
    return total


def outgoing_kernel(*refs):
    out_ref = refs[4]
    out_ref[...] = product_of(refs[:2], refs[2:4], slice(None)).astype(out_ref.dtype)


def outgoing(heads, weights, dtype):
    rows, depth = heads[0].shape
    cols = weights[0].shape[1]
    return pl.pallas_call(
        outgoing_kernel,
        out_shape=jax.ShapeDtypeStruct((rows, cols), dtype),
        in_specs=[VMEM] * 4,
        out_specs=VMEM,
        cost_estimate=pl.CostEstimate(
            flops=4 * rows * depth * cols, bytes_accessed=4 << 20, transcendentals=0
        ),
        compiler_params=limit(9),
        name="outgoing",
    )(*heads, *weights)


def quarter_kernel(count, info_ref, own_ref, got_ref, x_ref, fresh_ref, partner_ref, *refs):
    next_mine, next_other, quarter = refs
    me, place, bit_a, bit_b = whereabouts(info_ref, count)
    block, depth = fresh_ref.shape[0], own_ref.shape[1] // 2
    second = (me & bit_b) // bit_b
    here = pl.ds(pl.multiple_of(second * block, block), block)
    there = pl.ds(pl.multiple_of((1 - second) * block, block), block)
    for t in range(2):
        rows = slice(t * block, (t + 1) * block)
        at = pl.multiple_of(((me & bit_a) | (t * bit_b)) * block, block)
        x = x_ref[pl.ds(at, block), :].astype(F32)
        quarter[rows, :] = (x + own_ref[rows, :] + got_ref[rows, :].astype(F32)).astype(BF16)

    @pl.when(place == 1)
    def _():
        quarter[here, :] = fresh_ref[...]
        quarter[there, :] = partner_ref[...]

    part = (me & bit_a) // bit_a
    next_mine[...] = quarter[:, pl.ds(pl.multiple_of(part * depth, depth), depth)]
    next_other[...] = quarter[:, pl.ds(pl.multiple_of((1 - part) * depth, depth), depth)]


def quarter(info, count, own, got, x, fresh, fresh_partner):
    rows, cols = own.shape
    block = jax.ShapeDtypeStruct((rows, cols // 2), BF16)
    return pl.pallas_call(
        functools.partial(quarter_kernel, count),
        out_shape=(block, block),
        in_specs=[SMEM] + [VMEM] * 5,
        out_specs=(VMEM, VMEM),
        scratch_shapes=[pltpu.VMEM((rows, cols), BF16)],
        cost_estimate=pl.CostEstimate(
            flops=4 * rows * cols, bytes_accessed=4 << 20, transcendentals=0
        ),
        compiler_params=limit(9),
        name="quarter",
    )(info, own, got, x, fresh, fresh_partner)


def cross_kernel(count, info_ref, *refs):
    out_ref = refs[4]
    me, _, _, bit_b = whereabouts(info_ref, count)
    block = out_ref.shape[0]
    there = pl.multiple_of((1 - (me & bit_b) // bit_b) * block, block)
    out_ref[...] = product_of(refs[:2], refs[2:4], pl.ds(there, block)).astype(BF16)


def crossing(info, count, heads, weights):
    return pl.pallas_call(
        functools.partial(cross_kernel, count),
        out_shape=jax.ShapeDtypeStruct((heads[0].shape[0] // 2, weights[0].shape[1]), BF16),
        in_specs=[SMEM] + [VMEM] * 4,
        out_specs=VMEM,
        cost_estimate=pl.CostEstimate(
            flops=2 * heads[0].size * weights[0].shape[1],
            bytes_accessed=4 << 20,
            transcendentals=0,
        ),
        compiler_params=limit(9),
        name="crossing",
    )(info, *heads, *weights)


def deal_kernel(count, info_ref, *refs):
    other_refs, mine_refs, w_refs, x_ref = refs[:2], refs[2:4], refs[4:6], refs[6]
    keep_ref, a_ref, b_ref = refs[7:]
    me, _, _, bit_b = whereabouts(info_ref, count)
    block = keep_ref.shape[0]
    second = (me & bit_b) // bit_b
    for out_ref, part, offset in ((b_ref, 1 - second, bit_b), (keep_ref, second, 0)):
        at = pl.multiple_of((me ^ offset) * block, block)
        there = pl.ds(pl.multiple_of(part * block, block), block)
        out_ref[...] = product_of(mine_refs, w_refs, there) + x_ref[
            pl.ds(at, block), :
        ].astype(F32)
    here = pl.ds(pl.multiple_of(second * block, block), block)
    a_ref[:block, :] = product_of(other_refs, w_refs, here).astype(BF16)
    rows = 2 * block
    size, cols = mine_refs[0].shape[0] - rows, mine_refs[0].shape[1]
    fold = x_ref.shape[1] // cols
    high = size // fold
    for i, ref in enumerate(mine_refs):
        for q in range(fold):
            a_ref[block + i * high : block + (i + 1) * high, q * cols : (q + 1) * cols] = ref[
                rows + q * high : rows + (q + 1) * high, :
            ]


def deal(info, count, other, mine, weights, x):
    rows, cols = x.shape
    block = rows // count
    size = mine[0].shape[0] - 2 * block
    wide = jax.ShapeDtypeStruct((block, cols), F32)
    more = jax.ShapeDtypeStruct((block + 2 * size * mine[0].shape[1] // cols, cols), BF16)
    return pl.pallas_call(
        functools.partial(deal_kernel, count),
        out_shape=(wide, more, wide),
        in_specs=[SMEM] + [VMEM] * 7,
        out_specs=(VMEM,) * 3,
        cost_estimate=pl.CostEstimate(
            flops=3 * rows * mine[0].shape[1] * cols, bytes_accessed=4 << 20, transcendentals=0
        ),
        compiler_params=limit(12),
        name="deal",
    )(info, *other, *mine, *weights, x)


def combine_kernel(mine_ref, got_ref, out_ref):
    out_ref[...] = (mine_ref[...] + got_ref[...].astype(F32)).astype(BF16)


def combine(mine, got):
    return pl.pallas_call(
        combine_kernel,
        out_shape=jax.ShapeDtypeStruct(got.shape, BF16),
        in_specs=[VMEM, VMEM],
        out_specs=VMEM,
        compiler_params=limit(4),
        name="combine",
    )(mine, got)


def last_kernel(count, info_ref, keep_ref, a_ref, b_ref, heads_ref, *refs):
    resident_ref, own_ref, out_ref, final_ref = refs
    me, _, bit_a, bit_b = whereabouts(info_ref, count)
    block, width = out_ref.shape
    depth = width // count
    for t in range(2):
        columns = slice(t * depth, (t + 1) * depth)
        out = keep_ref[:, columns] + a_ref[:block, columns].astype(F32)
        for low, half in ((me & bit_b, out.astype(BF16)), ((me & bit_b) ^ bit_b, b_ref[:, columns])):
            at = pl.multiple_of((low | (t * bit_a)) * depth, depth)
            out_ref[:, pl.ds(at, depth)] = half
    own, size = own_ref.shape[0], own_ref.shape[1]
    cols = own * size
    fold = a_ref.shape[1] // cols
    high = size // fold
    rows = heads_ref.shape[0] - size
    for h in range(own):
        final_ref[me * own + h] = own_ref[h]
        columns = slice(h * size, (h + 1) * size)
        at = (me ^ bit_b) * own + h
        final_ref[at] = resident_ref[at] + heads_ref[rows:, columns].astype(F32)
        for i, offset in enumerate((bit_a, bit_a | bit_b)):
            at = (me ^ offset) * own + h
            for q in range(fold):
                inner = slice(q * high, (q + 1) * high)
                change = a_ref[
                    block + i * high : block + (i + 1) * high,
                    q * cols + h * size : q * cols + (h + 1) * size,
                ]
                final_ref[at, inner, :] = resident_ref[at, inner, :] + change.astype(F32)


def last(info, count, keep, from_a, from_b, heads_b, resident, own_state):
    block, half = keep.shape
    return pl.pallas_call(
        functools.partial(last_kernel, count),
        out_shape=(
            jax.ShapeDtypeStruct((block, 2 * half), BF16),
            jax.ShapeDtypeStruct(resident.shape, F32),
        ),
        in_specs=[SMEM] + [VMEM] * 6,
        out_specs=(VMEM, VMEM),
        cost_estimate=pl.CostEstimate(
            flops=4 * block * half, bytes_accessed=4 << 20, transcendentals=0
        ),
        compiler_params=limit(9),
        name="last",
    )(info, keep, from_a, from_b, heads_b, resident, own_state)


def paired_body(
    section_inputs, fresh_group, resident_state, qkv_weight, out_weight, input_gain, head_gain
):
    count = lax.axis_size("row")
    sections = lax.axis_size("section")
    row, section = lax.axis_index("row"), lax.axis_index("section")
    place = jnp.where(section == 0, 2, jnp.where(section == sections - 1, 1, 0))
    info = (row + count * (place + 3 * (section % 2))).astype(jnp.int32)[None]
    x, resident, width = section_inputs[0], resident_state[0], input_gain.shape[1]

    own_half, other_half = halve(info, count, x)
    from_b = along(other_half, 1)
    from_a = along(own_half, 0)
    mine, partner, mine_b, partner_b = cut(info, qkv_weight[0], count)
    partner_b = along(partner_b, 0)
    from_far = along(from_b, 0)
    partner = along(partner, 0)
    out_own, out_other, fresh_own, fresh_other = halve(
        info, count, out_weight[0], fresh_group
    )
    outs_b = along(out_other, 1)
    fresh_partner = along(fresh_other, 1, sections - 1)
    given, scaled, rows, columns_b = given_product(
        info,
        count,
        input_gain,
        [own_half, from_a, from_b, from_far],
        [mine_b, partner_b],
    )
    got = along(given, 1)
    own, columns = own_product(info, count, scaled, [mine, partner])
    other, mine, own_state = attend(info, count, width, own, given, got, resident, head_gain)
    other_b = along(other, 1)
    mine_b = along(mine, 1)
    out_pair = [out_own, outs_b]
    given_out = outgoing([other, other_b], out_pair, BF16)
    got_out = along(given_out, 0)
    own_out = outgoing([mine, mine_b], out_pair, F32)
    next_mine, next_other = quarter(info, count, own_out, got_out, rows, fresh_own, fresh_partner)
    from_b = to_next(next_other, 0, 1)
    from_a = to_next(next_mine, 1, 0)
    own_half = to_next(next_mine, 0, 0)
    from_far = along(from_b, 0)
    given, scaled, rows = given_product(
        info, count, input_gain, [own_half, from_a, from_b, from_far], [columns_b]
    )
    got = along(given, 1)
    (own,) = own_product(info, count, scaled, [columns])
    other, mine, own_state = attend(
        info, count, width, own, given, got, own_state, head_gain, resident
    )
    other_b = along(other, 1)
    mine_b = along(mine, 1)
    cross = crossing(info, count, [other, other_b], out_pair)
    cross = along(cross, 0)
    keep, to_a, to_b = deal(
        info, count, [other, other_b], [mine, mine_b], out_pair, rows
    )
    from_a = along(to_a, 0)
    to_b = combine(to_b, cross)
    from_b = along(to_b, 1)
    second_out, final_state = last(info, count, keep, from_a, from_b, mine_b, resident, own_state)
    return (second_out[None], final_state[None])


def solution(mesh):
    in_specs = (
        P("section", "row", None),
        P("row", None),
        P("section", None, None, None),
        P("section", "row", None),
        P("section", "row", None),
        P("section", None),
        P("section", None),
    )
    out_specs = (P("section", "row", None), P("section", None, None, None))

    def whole(*args):
        count = mesh.shape["row"]
        heads, size = args[2].shape[1:3]
        block = args[0].shape[1] // count
        paired = count == 4 and mesh.shape["section"] % 2 == 0 and heads % count == 0
        paired = paired and block * count <= 3 * heads // count * size
        body = paired_body if paired else gathered_body
        return jax.shard_map(
            body, mesh=mesh, in_specs=in_specs, out_specs=out_specs, check_vma=False
        )(*args)

    return whole
```

```python
import functools

import jax
import jax.numpy as jnp
from jax import lax
from jax.experimental import pallas as pl
from jax.experimental.pallas import tpu as pltpu
from jax.sharding import PartitionSpec as P


VMEM = pl.BlockSpec(memory_space=pltpu.VMEM)
SMEM = pl.BlockSpec(memory_space=pltpu.SMEM)
F32 = jnp.float32
BF16 = jnp.bfloat16


def passed_along(value, axis, by):
    peers = lax.axis_size(axis)
    pairs = [(i, i + by) for i in range(peers) if 0 <= i + by < peers]
    return lax.ppermute(value, axis, pairs)


def layer(inputs, state, qkv_full, out_full, input_gain, head_gain):
    rows = inputs.shape[0]
    heads = state.shape[0]
    head_size = state.shape[1]
    width = heads * head_size
    highest = lax.Precision.HIGHEST
    wide = inputs.astype(F32)
    normed = (
        wide * lax.rsqrt(jnp.mean(wide * wide, axis=-1, keepdims=True) + 1e-05) * input_gain
    ).astype(BF16)
    projected = jnp.dot(normed, qkv_full, preferred_element_type=F32)
    queries = jax.nn.silu(projected[:, :width]).astype(BF16).reshape(rows, heads, head_size)
    key_rows = (
        jax.nn.silu(projected[:, width : 2 * width]).astype(BF16).reshape(rows, heads, head_size)
    )
    value_rows = projected[:, 2 * width :].astype(BF16).reshape(rows, heads, head_size)
    own_state = jnp.einsum("jhd,jhe->hde", key_rows, value_rows, preferred_element_type=F32)
    every = lax.all_gather(own_state[None].astype(BF16), "row", axis=0, tiled=True).astype(F32)
    order = lax.iota(jnp.int32, every.shape[0])
    earlier = (order < lax.axis_index("row")).astype(F32)
    before = jnp.sum(every * earlier[:, None, None, None], axis=0)
    total = jnp.sum(every, axis=0)
    prefix = state + before
    carried = jnp.einsum("ihd,hde->ihe", queries.astype(F32), prefix, precision=highest)
    scores = jnp.einsum("ihd,jhd->hij", queries, key_rows, preferred_element_type=F32)
    causal = lax.broadcasted_iota(jnp.int32, (rows, rows), 0) >= lax.broadcasted_iota(
        jnp.int32, (rows, rows), 1
    )
    weights = jnp.where(causal[None], scores, 0.0).astype(BF16)
    local = jnp.einsum("hij,jhe->ihe", weights, value_rows, preferred_element_type=F32)
    attended = carried + local
    scaled = attended * lax.rsqrt(jnp.mean(attended * attended, axis=-1, keepdims=True) + 1e-06)
    head_out = (scaled.reshape(rows, width) * head_gain).astype(BF16)
    result = (wide + jnp.dot(head_out, out_full, preferred_element_type=F32)).astype(BF16)
    return (result, state + total)


def gathered_body(
    section_inputs, fresh_group, resident_state, qkv_weight, out_weight, input_gain, head_gain
):
    qkv_full, out_full = (
        lax.all_gather(qkv_weight[0], "row", axis=0, tiled=True),
        lax.all_gather(out_weight[0], "row", axis=0, tiled=True),
    )
    first_out, first_state = layer(
        section_inputs[0], resident_state[0], qkv_full, out_full, input_gain[0], head_gain[0]
    )
    arrived = passed_along(first_out, "section", 1)
    second_in = jnp.where(lax.axis_index("section") == 0, fresh_group, arrived)
    second_out, second_state = layer(
        second_in, first_state, qkv_full, out_full, input_gain[0], head_gain[0]
    )
    return (second_out[None], second_state[None])


def steps(section):
    return (1, 2) if section % 2 == 0 else (2, 1)


def along(value, axis, only=None):
    sections, rows = lax.axis_size("section"), lax.axis_size("row")
    pairs = [
        (s * rows + r, s * rows + (r ^ steps(s)[axis]))
        for s in range(sections)
        for r in range(rows)
        if only is None or s == only
    ]
    return lax.ppermute(value, ("section", "row"), pairs)


def to_next(value, over_a, over_b):
    sections, rows = lax.axis_size("section"), lax.axis_size("row")
    pairs = []
    for s in range(sections):
        to = (s + 1) % sections
        a, b = steps(to)
        pairs += [(s * rows + r, to * rows + (r ^ (a * over_a) ^ (b * over_b))) for r in range(rows)]
    return lax.ppermute(value, ("section", "row"), pairs)


def limit(mebibytes):
    return pltpu.CompilerParams(vmem_limit_bytes=mebibytes << 20)


def whereabouts(info_ref, count):
    info = info_ref[0]
    odd = info // (3 * count)
    return info % count, info // count % 3, 1 + odd, 2 - odd


def halve_kernel(count, info_ref, *refs):
    me, _, bit_a, bit_b = whereabouts(info_ref, count)
    sources, outs = refs[: len(refs) // 3], refs[len(refs) // 3 :]
    for i, source in enumerate(sources):
        depth = source.shape[1] // count
        for out_ref, low in zip(outs[2 * i :], (me & bit_b, (me & bit_b) ^ bit_b)):
            for part, block in enumerate((low, low | bit_a)):
                at = pl.multiple_of(block * depth, depth)
                out_ref[:, part * depth : (part + 1) * depth] = source[:, pl.ds(at, depth)]


def halve(info, count, *arrays):
    outs = [
        jax.ShapeDtypeStruct((x.shape[0], x.shape[1] // 2), x.dtype)
        for x in arrays
        for _ in range(2)
    ]
    return pl.pallas_call(
        functools.partial(halve_kernel, count),
        out_shape=outs,
        in_specs=[SMEM] + [VMEM] * len(arrays),
        out_specs=[VMEM] * len(outs),
        compiler_params=limit(6),
        name="halve",
    )(info, *arrays)


def cut_kernel(count, info_ref, w_ref, *out_refs):
    me, _, bit_a, bit_b = whereabouts(info_ref, count)
    cols = out_refs[0].shape[1] // 3
    for out_ref, offset in zip(out_refs, (0, bit_a, bit_b, bit_a | bit_b)):
        for c in range(3):
            at = pl.multiple_of((c * count + (me ^ offset)) * cols, cols)
            out_ref[:, c * cols : (c + 1) * cols] = w_ref[:, pl.ds(at, cols)]


def cut(info, weight, count):
    depth, cols3 = weight.shape
    return pl.pallas_call(
        functools.partial(cut_kernel, count),
        out_shape=[jax.ShapeDtypeStruct((depth, cols3 // count), BF16)] * 4,
        in_specs=[SMEM, VMEM],
        out_specs=[VMEM] * 4,
        compiler_params=limit(9),
        name="cut",
    )(info, weight)


def assemble(me, bit_a, bit_b, x_refs, x_all):
    offsets = (0, bit_a, bit_b, bit_a | bit_b)
    rows, width = x_refs[0].shape
    if width == x_all.shape[1]:
        for x_ref, offset in zip(x_refs, offsets):
            x_all[pl.ds(pl.multiple_of((me ^ offset) * rows, rows), rows), :] = x_ref[...]
        return
    block = rows // 2
    for j, x_ref in enumerate(x_refs):
        part = (me & bit_a) // bit_a
        columns = pl.ds(pl.multiple_of((part if j % 2 == 0 else 1 - part) * width, width), width)
        low = me & bit_b if j < 2 else (me & bit_b) ^ bit_b
        for t in range(2):
            at = pl.multiple_of((low | (t * bit_a)) * block, block)
            x_all[pl.ds(at, block), columns] = x_ref[t * block : (t + 1) * block, :]


def pair_weights(me, bit_a, w_refs, w_all):
    depth = w_refs[0].shape[0]
    second = (me & bit_a) // bit_a
    w_all[pl.ds(pl.multiple_of(second * depth, depth), depth), :] = w_refs[0][...]
    w_all[pl.ds(pl.multiple_of((1 - second) * depth, depth), depth), :] = w_refs[1][...]


def given_kernel(count, first, info_ref, gain_ref, *refs):
    me, _, bit_a, bit_b = whereabouts(info_ref, count)
    x_refs, refs = refs[:4], refs[4:]
    w_refs, refs = refs[: 1 + first], refs[1 + first :]
    out_ref, scaled_ref, x_all, refs = *refs[:3], refs[3:]
    w_all = refs[0] if first else w_refs[0]
    assemble(me, bit_a, bit_b, x_refs, x_all)
    if first:
        pair_weights(me, bit_a, w_refs, w_all)
    depth = scaled_ref.shape[1] // 2
    rows, tail = x_all.shape[0], out_ref.shape[0] - x_all.shape[0]
    total = None
    for part in range(2):
        at = pl.multiple_of(((me & bit_b) | (part * bit_a)) * depth, depth)
        columns = slice(part * depth, (part + 1) * depth)
        wide = x_all[:, columns].astype(F32)
        scaled_ref[:, columns] = (wide * gain_ref[:, pl.ds(at, depth)]).astype(BF16)
        term = lax.dot_general(
            jnp.ones((tail, depth), BF16),
            (wide * wide).astype(BF16),
            (((1,), (1,)), ((), ())),
            preferred_element_type=F32,
        )
        total = term if total is None else total + term
    out_ref[:rows, :] = jnp.dot(
        scaled_ref[...], w_all[...], preferred_element_type=F32
    ).astype(BF16)
    high = total.astype(BF16).astype(F32)
    line = lax.broadcasted_iota(jnp.int32, total.shape, 0)
    pair = jnp.where(line == 0, high, jnp.where(line == 1, total - high, 0.0))
    out_ref[rows:, :] = jnp.zeros((tail, out_ref.shape[1]), BF16)
    out_ref[rows:, :rows] = pair.astype(BF16)


def given_product(info, count, gain, x, w):
    first = len(w) > 1
    rows, half = x[0].size * len(x) * 2 // gain.shape[1], gain.shape[1] // 2
    cols = w[0].shape[1]
    outs = [jax.ShapeDtypeStruct((rows + 16, cols), BF16)]
    outs += [jax.ShapeDtypeStruct((rows, half), BF16)] * 2
    outs += [jax.ShapeDtypeStruct((half, cols), BF16)] if first else []
    return pl.pallas_call(
        functools.partial(given_kernel, count, first),
        out_shape=outs,
        in_specs=[SMEM] + [VMEM] * (1 + len(x) + len(w)),
        out_specs=[VMEM] * len(outs),
        cost_estimate=pl.CostEstimate(
            flops=2 * rows * half * cols, bytes_accessed=4 << 20, transcendentals=0
        ),
        compiler_params=limit(12),
        name="given_first" if first else "given_second",
    )(info, gain, *x, *w)


def own_kernel(count, first, info_ref, scaled_ref, *refs):
    me, _, bit_a, _ = whereabouts(info_ref, count)
    w_refs, refs = refs[: 1 + first], refs[1 + first :]
    out_ref = refs[0]
    w_all = refs[1] if first else w_refs[0]
    if first:
        pair_weights(me, bit_a, w_refs, w_all)
    out_ref[...] = jnp.dot(scaled_ref[...], w_all[...], preferred_element_type=F32)


def own_product(info, count, scaled, w):
    first = len(w) > 1
    rows, half = scaled.shape
    cols = w[0].shape[1]
    outs = [jax.ShapeDtypeStruct((rows, cols), F32)]
    outs += [jax.ShapeDtypeStruct((half, cols), BF16)] if first else []
    return pl.pallas_call(
        functools.partial(own_kernel, count, first),
        out_shape=outs,
        in_specs=[SMEM] + [VMEM] * (1 + len(w)),
        out_specs=[VMEM] * len(outs),
        cost_estimate=pl.CostEstimate(
            flops=2 * rows * half * cols, bytes_accessed=4 << 20, transcendentals=0
        ),
        compiler_params=limit(12),
        name="own_first" if first else "own_second",
    )(info, scaled, *w)


def attend_kernel(count, first, width, info_ref, *refs):
    own_ref, given_ref, got_ref, state_ref, gain_ref, refs = *refs[:5], refs[5:]
    if not first:
        resident_ref, refs = refs[0], refs[1:]
    other_ref, mine_ref, new_state_ref, qkv, ho_all = refs
    me, _, bit_a, bit_b = whereabouts(info_ref, count)
    own, size = new_state_ref.shape[0], new_state_ref.shape[1]
    cols = own * size
    block = own_ref.shape[0] // count
    rows, square = own_ref.shape[0], None
    for ref in (given_ref, got_ref):
        tail = ref[rows:, :rows]
        term = lax.dot_general(
            tail,
            jnp.ones((tail.shape[0], 128), BF16),
            (((0,), (0,)), ((), ())),
            preferred_element_type=F32,
        )
        square = term if square is None else square + term
    scale = lax.rsqrt(square[:, :1] / width + 1e-05)
    for c in range(3):
        columns = slice(c * cols, (c + 1) * cols)
        part = (own_ref[:, columns] + got_ref[:rows, columns].astype(F32)) * scale
        if c < 2:
            part = part / (1.0 + jnp.exp(-part))
        qkv[:, columns] = part.astype(BF16)
    causal = lax.broadcasted_iota(jnp.int32, (block, block), 0) >= lax.broadcasted_iota(
        jnp.int32, (block, block), 1
    )
    gains = gain_ref[:, pl.ds(pl.multiple_of(me * cols, cols), cols)]
    for h in range(own):
        prefix = state_ref[me * own + h] if first else state_ref[h]
        for b in range(count):
            rows = slice(b * block, (b + 1) * block)
            q, k, v = (
                qkv[rows, c * cols + h * size : c * cols + (h + 1) * size] for c in range(3)
            )
            high = prefix.astype(BF16)
            low = (prefix - high.astype(F32)).astype(BF16)
            scores = lax.dot_general(
                q, k, (((1,), (1,)), ((), ())), preferred_element_type=F32
            )
            weights = jnp.where(causal, scores, 0.0).astype(BF16)
            attended = (
                jnp.dot(q, high, preferred_element_type=F32)
                + jnp.dot(q, low, preferred_element_type=F32)
                + jnp.dot(weights, v, preferred_element_type=F32)
            )
            mean = jnp.mean(attended * attended, axis=-1, keepdims=True)
            scaled = attended * lax.rsqrt(mean + 1e-06) * gains[:, h * size : (h + 1) * size]
            ho_all[rows, h * size : (h + 1) * size] = scaled.astype(BF16)
            prefix = prefix + lax.dot_general(
                k, v, (((0,), (0,)), ((), ())), preferred_element_type=F32
            )
        new_state_ref[h] = prefix
        if not first:
            change = (prefix - resident_ref[me * own + h]).astype(BF16)
            mine_ref[2 * block :, h * size : (h + 1) * size] = change
    for ref, low in ((other_ref, (me & bit_a) ^ bit_a), (mine_ref, me & bit_a)):
        for t in range(2):
            at = pl.multiple_of((low | (t * bit_b)) * block, block)
            ref[t * block : (t + 1) * block, :] = ho_all[pl.ds(at, block), :]


def attend(info, count, width, own, given, got, state, head_gain, resident=None):
    first = resident is None
    rows, cols3 = own.shape
    size = state.shape[-1]
    heads = cols3 // 3 // size
    ins = [info, own, given, got, state, head_gain] + ([] if first else [resident])
    outs = [
        jax.ShapeDtypeStruct((rows // 2, heads * size), BF16),
        jax.ShapeDtypeStruct((rows // 2 + (0 if first else size), heads * size), BF16),
        jax.ShapeDtypeStruct((heads, size, size), F32),
    ]
    return pl.pallas_call(
        functools.partial(attend_kernel, count, first, width),
        out_shape=outs,
        in_specs=[SMEM] + [VMEM] * (len(ins) - 1),
        out_specs=[VMEM] * len(outs),
        scratch_shapes=[
            pltpu.VMEM((rows, cols3), BF16),
            pltpu.VMEM((rows, heads * size), BF16),
        ],
        cost_estimate=pl.CostEstimate(
            flops=10 * rows * heads * size * size, bytes_accessed=8 << 20, transcendentals=0
        ),
        compiler_params=limit(15),
        name="attend_first" if first else "attend_second",
    )(*ins)


def product_of(ho_refs, w_refs, rows):
    total = None
    for ho_ref, w_ref in zip(ho_refs, w_refs):
        term = jnp.dot(ho_ref[rows, :], w_ref[...], preferred_element_type=F32)
        total = term if total is None else total + term
    return total


def outgoing_kernel(count, parts, info_ref, *refs):
    me, _, bit_a, _ = whereabouts(info_ref, count)
    ho_refs, w_refs, outs = refs[:2], refs[2:4], refs[4:]
    if parts == 1:
        outs[0][...] = product_of(ho_refs, w_refs, slice(None)).astype(outs[0].dtype)
        return
    width = outs[0].shape[1]
    second = (me & bit_a) // bit_a
    for out_ref, part in ((outs[0], second), (outs[1], 1 - second)):
        columns = pl.ds(pl.multiple_of(part * width, width), width)
        total = None
        for ho_ref, w_ref in zip(ho_refs, w_refs):
            term = jnp.dot(ho_ref[...], w_ref[:, columns], preferred_element_type=F32)
            total = term if total is None else total + term
        out_ref[...] = total.astype(out_ref.dtype)


def outgoing(info, count, heads, weights, dtype, parts):
    rows, depth = heads[0].shape
    cols = weights[0].shape[1]
    return pl.pallas_call(
        functools.partial(outgoing_kernel, count, parts),
        out_shape=[jax.ShapeDtypeStruct((rows, cols // parts), dtype)] * parts,
        in_specs=[SMEM] + [VMEM] * 4,
        out_specs=[VMEM] * parts,
        cost_estimate=pl.CostEstimate(
            flops=4 * rows * depth * cols, bytes_accessed=4 << 20, transcendentals=0
        ),
        compiler_params=limit(9),
        name="outgoing_mine" if parts == 1 else "outgoing_given",
    )(info, *heads, *weights)


def quarter_kernel(count, mine, info_ref, own_ref, got_ref, x_ref, fresh_ref, partner_ref, out_ref):
    me, place, bit_a, bit_b = whereabouts(info_ref, count)
    block, depth = fresh_ref.shape[0], out_ref.shape[1]
    part = (me & bit_a) // bit_a
    part = part if mine else 1 - part
    columns = pl.ds(pl.multiple_of(part * depth, depth), depth)
    for t in range(2):
        rows = slice(t * block, (t + 1) * block)
        at = pl.multiple_of(((me & bit_a) | (t * bit_b)) * block, block)
        x = x_ref[pl.ds(at, block), columns].astype(F32)
        out_ref[rows, :] = (x + own_ref[rows, columns] + got_ref[rows, :].astype(F32)).astype(BF16)

    @pl.when(place == 1)
    def _():
        second = (me & bit_b) // bit_b
        here = pl.ds(pl.multiple_of(second * block, block), block)
        there = pl.ds(pl.multiple_of((1 - second) * block, block), block)
        out_ref[here, :] = fresh_ref[:, columns]
        out_ref[there, :] = partner_ref[:, columns]


def quarter(info, count, own, got, x, fresh, fresh_partner, mine):
    return pl.pallas_call(
        functools.partial(quarter_kernel, count, mine),
        out_shape=jax.ShapeDtypeStruct(got.shape, BF16),
        in_specs=[SMEM] + [VMEM] * 5,
        out_specs=VMEM,
        cost_estimate=pl.CostEstimate(
            flops=4 * got.size, bytes_accessed=4 << 20, transcendentals=0
        ),
        compiler_params=limit(9),
        name="quarter_mine" if mine else "quarter_other",
    )(info, own, got, x, fresh, fresh_partner)


def cross_kernel(count, info_ref, *refs):
    out_ref = refs[4]
    me, _, _, bit_b = whereabouts(info_ref, count)
    block = out_ref.shape[0]
    there = pl.multiple_of((1 - (me & bit_b) // bit_b) * block, block)
    out_ref[...] = product_of(refs[:2], refs[2:4], pl.ds(there, block)).astype(BF16)


def crossing(info, count, heads, weights):
    return pl.pallas_call(
        functools.partial(cross_kernel, count),
        out_shape=jax.ShapeDtypeStruct((heads[0].shape[0] // 2, weights[0].shape[1]), BF16),
        in_specs=[SMEM] + [VMEM] * 4,
        out_specs=VMEM,
        cost_estimate=pl.CostEstimate(
            flops=2 * heads[0].size * weights[0].shape[1],
            bytes_accessed=4 << 20,
            transcendentals=0,
        ),
        compiler_params=limit(9),
        name="crossing",
    )(info, *heads, *weights)


def deal_kernel(count, info_ref, *refs):
    other_refs, mine_refs, w_refs, x_ref = refs[:2], refs[2:4], refs[4:6], refs[6]
    keep_ref, a_ref, b_ref = refs[7:]
    me, _, _, bit_b = whereabouts(info_ref, count)
    block = keep_ref.shape[0]
    second = (me & bit_b) // bit_b
    for out_ref, part, offset in ((b_ref, 1 - second, bit_b), (keep_ref, second, 0)):
        at = pl.multiple_of((me ^ offset) * block, block)
        there = pl.ds(pl.multiple_of(part * block, block), block)
        out_ref[...] = product_of(mine_refs, w_refs, there) + x_ref[
            pl.ds(at, block), :
        ].astype(F32)
    here = pl.ds(pl.multiple_of(second * block, block), block)
    a_ref[:block, :] = product_of(other_refs, w_refs, here).astype(BF16)
    rows = 2 * block
    size, cols = mine_refs[0].shape[0] - rows, mine_refs[0].shape[1]
    fold = x_ref.shape[1] // cols
    high = size // fold
    for i, ref in enumerate(mine_refs):
        for q in range(fold):
            a_ref[block + i * high : block + (i + 1) * high, q * cols : (q + 1) * cols] = ref[
                rows + q * high : rows + (q + 1) * high, :
            ]


def deal(info, count, other, mine, weights, x):
    rows, cols = x.shape
    block = rows // count
    size = mine[0].shape[0] - 2 * block
    wide = jax.ShapeDtypeStruct((block, cols), F32)
    more = jax.ShapeDtypeStruct((block + 2 * size * mine[0].shape[1] // cols, cols), BF16)
    return pl.pallas_call(
        functools.partial(deal_kernel, count),
        out_shape=(wide, more, wide),
        in_specs=[SMEM] + [VMEM] * 7,
        out_specs=(VMEM,) * 3,
        cost_estimate=pl.CostEstimate(
            flops=3 * rows * mine[0].shape[1] * cols, bytes_accessed=4 << 20, transcendentals=0
        ),
        compiler_params=limit(12),
        name="deal",
    )(info, *other, *mine, *weights, x)


def combine_kernel(mine_ref, got_ref, out_ref):
    out_ref[...] = (mine_ref[...] + got_ref[...].astype(F32)).astype(BF16)


def combine(mine, got):
    return pl.pallas_call(
        combine_kernel,
        out_shape=jax.ShapeDtypeStruct(got.shape, BF16),
        in_specs=[VMEM, VMEM],
        out_specs=VMEM,
        compiler_params=limit(4),
        name="combine",
    )(mine, got)


def last_kernel(count, info_ref, keep_ref, a_ref, b_ref, heads_ref, *refs):
    resident_ref, own_ref, out_ref, final_ref = refs
    me, _, bit_a, bit_b = whereabouts(info_ref, count)
    block, width = out_ref.shape
    depth = width // count
    for t in range(2):
        columns = slice(t * depth, (t + 1) * depth)
        out = keep_ref[:, columns] + a_ref[:block, columns].astype(F32)
        for low, half in ((me & bit_b, out.astype(BF16)), ((me & bit_b) ^ bit_b, b_ref[:, columns])):
            at = pl.multiple_of((low | (t * bit_a)) * depth, depth)
            out_ref[:, pl.ds(at, depth)] = half
    own, size = own_ref.shape[0], own_ref.shape[1]
    cols = own * size
    fold = a_ref.shape[1] // cols
    high = size // fold
    rows = heads_ref.shape[0] - size
    for h in range(own):
        final_ref[me * own + h] = own_ref[h]
        columns = slice(h * size, (h + 1) * size)
        at = (me ^ bit_b) * own + h
        final_ref[at] = resident_ref[at] + heads_ref[rows:, columns].astype(F32)
        for i, offset in enumerate((bit_a, bit_a | bit_b)):
            at = (me ^ offset) * own + h
            for q in range(fold):
                inner = slice(q * high, (q + 1) * high)
                change = a_ref[
                    block + i * high : block + (i + 1) * high,
                    q * cols + h * size : q * cols + (h + 1) * size,
                ]
                final_ref[at, inner, :] = resident_ref[at, inner, :] + change.astype(F32)


def last(info, count, keep, from_a, from_b, heads_b, resident, own_state):
    block, half = keep.shape
    return pl.pallas_call(
        functools.partial(last_kernel, count),
        out_shape=(
            jax.ShapeDtypeStruct((block, 2 * half), BF16),
            jax.ShapeDtypeStruct(resident.shape, F32),
        ),
        in_specs=[SMEM] + [VMEM] * 6,
        out_specs=(VMEM, VMEM),
        cost_estimate=pl.CostEstimate(
            flops=4 * block * half, bytes_accessed=4 << 20, transcendentals=0
        ),
        compiler_params=limit(9),
        name="last",
    )(info, keep, from_a, from_b, heads_b, resident, own_state)


def paired_body(
    section_inputs, fresh_group, resident_state, qkv_weight, out_weight, input_gain, head_gain
):
    count = lax.axis_size("row")
    sections = lax.axis_size("section")
    row, section = lax.axis_index("row"), lax.axis_index("section")
    place = jnp.where(section == 0, 2, jnp.where(section == sections - 1, 1, 0))
    info = (row + count * (place + 3 * (section % 2))).astype(jnp.int32)[None]
    x, resident, width = section_inputs[0], resident_state[0], input_gain.shape[1]

    own_half, other_half = halve(info, count, x)
    from_b = along(other_half, 1)
    from_a = along(own_half, 0)
    mine, partner, mine_b, partner_b = cut(info, qkv_weight[0], count)
    partner_b = along(partner_b, 0)
    from_far = along(from_b, 0)
    partner = along(partner, 0)
    out_own, out_other, fresh_own, fresh_other = halve(
        info, count, out_weight[0], fresh_group
    )
    outs_b = along(out_other, 1)
    fresh_partner = along(fresh_other, 1, sections - 1)
    given, scaled, rows, columns_b = given_product(
        info,
        count,
        input_gain,
        [own_half, from_a, from_b, from_far],
        [mine_b, partner_b],
    )
    got = along(given, 1)
    own, columns = own_product(info, count, scaled, [mine, partner])
    other, mine, own_state = attend(info, count, width, own, given, got, resident, head_gain)
    other_b = along(other, 1)
    mine_b = along(mine, 1)
    out_pair = [out_own, outs_b]
    given_out, given_late = outgoing(info, count, [other, other_b], out_pair, BF16, 2)
    got_out = along(given_out, 0)
    got_late = along(given_late, 0)
    (own_out,) = outgoing(info, count, [mine, mine_b], out_pair, F32, 1)
    residual = (rows, fresh_own, fresh_partner)
    next_other = quarter(info, count, own_out, got_out, *residual, mine=False)
    from_b = to_next(next_other, 0, 1)
    next_mine = quarter(info, count, own_out, got_late, *residual, mine=True)
    from_a = to_next(next_mine, 1, 0)
    own_half = to_next(next_mine, 0, 0)
    from_far = along(from_b, 0)
    given, scaled, rows = given_product(
        info, count, input_gain, [own_half, from_a, from_b, from_far], [columns_b]
    )
    got = along(given, 1)
    (own,) = own_product(info, count, scaled, [columns])
    other, mine, own_state = attend(
        info, count, width, own, given, got, own_state, head_gain, resident
    )
    other_b = along(other, 1)
    mine_b = along(mine, 1)
    cross = crossing(info, count, [other, other_b], out_pair)
    cross = along(cross, 0)
    keep, to_a, to_b = deal(
        info, count, [other, other_b], [mine, mine_b], out_pair, rows
    )
    from_a = along(to_a, 0)
    to_b = combine(to_b, cross)
    from_b = along(to_b, 1)
    second_out, final_state = last(info, count, keep, from_a, from_b, mine_b, resident, own_state)
    return (second_out[None], final_state[None])


def solution(mesh):
    in_specs = (
        P("section", "row", None),
        P("row", None),
        P("section", None, None, None),
        P("section", "row", None),
        P("section", "row", None),
        P("section", None),
        P("section", None),
    )
    out_specs = (P("section", "row", None), P("section", None, None, None))

    def whole(*args):
        count = mesh.shape["row"]
        heads, size = args[2].shape[1:3]
        block = args[0].shape[1] // count
        paired = count == 4 and mesh.shape["section"] % 2 == 0 and heads % count == 0
        paired = paired and block * count <= 3 * heads // count * size
        body = paired_body if paired else gathered_body
        return jax.shard_map(
            body, mesh=mesh, in_specs=in_specs, out_specs=out_specs, check_vma=False
        )(*args)

    return whole
```
